128 devices in a mesh: lon: 16 (over x_lo, z, core), lat: 8 (over y, x_hi).
Axes of the slice: x: 4 (x_hi: 2, x_lo: 2; x = x_hi * 2 + x_lo), y: 4, z: 4, core: 2. Of those that a mesh axis runs over, the one named last changes fastest.
Arguments:
- height: float32 [1, 1152, 4096], P(None, 'lat', 'lon'), may hold values from -6 to 6
- response: float32 [640], replicated, may hold values from 0.25 to 4
Outputs:
- loading: float32 [1, 1152, 4096], P(None, 'lat', 'lon')
The draws below stay inside these ranges and needn't reach their ends.
All inputs are finite; a program needn't handle non-finite values.
Results may differ from the reference program's by a relative error of at most 0.00085.
Values sent between devices are 32-bit elements; how exact they have to be, the bound alone decides.
No kernel may reach another device: no remote copies, remote signals or barrier semaphores. Data moves between devices by JAX's collectives and lax.ppermute only.
A program may use at most 64 MiB of HBM per device.

```python
import math
import jax
import jax.numpy as jnp
from jax import lax

NLAT = 1152
NLON = 4096
MODES = 640
FIELDS = 1


def block_scale(stream_key, shape, split, least, high):
    loudness = 1.0
    for dim, parts in split:
        draws = jax.random.uniform(jax.random.fold_in(jax.random.fold_in(stream_key, 6), dim), (parts,), jnp.float32, least / len(split), high / len(split))
        loudness = loudness * jnp.repeat(jnp.exp(draws), shape[dim] // parts).reshape((-1,) + (1,) * (len(shape) - 1 - dim))
    return loudness


def centred(key, extent, width, reach, split=(), held_as=jnp.bfloat16):
    array = jax.random.normal(key, extent, jnp.float32) * width
    if len(split) > 0:
        array = block_scale(key, extent, split, -0.22, 0.18) * array
    return jnp.clip(array, min=-reach, max=reach).astype(held_as)


def setup_inputs(seed: int = 0) -> dict:
    splits = jax.random.split(jax.random.key(seed), 3)
    return {
        "height": centred(splits[0], (FIELDS, NLAT, NLON), 1.0, 6.0, ((1, 8), (2, 16)), jnp.float32),
        "response": jnp.clip(jnp.exp(jax.random.uniform(splits[1], (MODES,), jnp.float32, math.log(0.25), math.log(4.0))), 0.25, 4.0),
    }


block_degrees = 64
rescale_every = 8
highest = lax.Precision.HIGHEST

def colatitude_parts(latitudes):
    colatitude = (latitudes.astype(jnp.float32) + 0.5) * (jnp.pi / NLAT)
    sines = jnp.sin(colatitude)
    return (jnp.cos(colatitude), sines, sines * (jnp.pi / NLAT))

def legendre_sweep(cosines, sines, orders, consume, initial):
    order_float = orders.astype(jnp.float32)
    log_start = 0.5 * (lax.lgamma(order_float + 1.5) - lax.lgamma(order_float + 1.0) - lax.lgamma(jnp.full_like(order_float, 1.5))) - 0.5 * jnp.log(4.0 * jnp.pi)
    log_scale = log_start[:, None] + order_float[:, None] * jnp.log(sines)[None, :]
    zero_field = jnp.zeros(log_scale.shape, jnp.float32)

    def one_block(block_index, carried):
        earlier, latest, log_scale, running = carried
        first_degree = (block_index * block_degrees).astype(jnp.int32)
        factor = jnp.exp(log_scale)
        layers = []
        for offset in range(block_degrees):
            degree = first_degree + offset
            started = degree > orders
            starting = degree == orders
            degree_float = degree.astype(jnp.float32)
            lower_float = degree_float - 1.0
            square_gap = jnp.where(started, degree_float * degree_float - order_float * order_float, 1.0)
            growth = jnp.sqrt(jnp.where(started, (4.0 * degree_float * degree_float - 1.0) / square_gap, 0.0))
            damping = jnp.sqrt(jnp.where(started, (lower_float * lower_float - order_float * order_float) / jnp.maximum(4.0 * lower_float * lower_float - 1.0, 1.0), 0.0))
            current = jnp.where(starting[:, None], 1.0, growth[:, None] * (cosines[None, :] * latest - damping[:, None] * earlier))
            layers.append(current * factor)
            earlier, latest = (latest, current)
            if (offset + 1) % rescale_every == 0:
                largest = jnp.maximum(jnp.maximum(jnp.abs(earlier), jnp.abs(latest)), 1.0)
                earlier = earlier / largest
                latest = latest / largest
                log_scale = log_scale + jnp.log(largest)
                factor = jnp.exp(log_scale)
        legendre = jnp.stack(layers)
        return (earlier, latest, log_scale, consume(running, legendre, first_degree))
    carried = (zero_field, zero_field, log_scale, initial)
    carried = lax.fori_loop(0, MODES // block_degrees, one_block, carried)
    return carried[3]

def analyse(spectrum, latitudes, orders):
    cosines, sines, weights = colatitude_parts(latitudes)
    weighted = spectrum * weights

    def consume(coefficients, legendre, first_degree):
        block_terms = jnp.einsum('lmj,mcfj->lmcf', legendre, weighted, precision=highest)
        return lax.dynamic_update_slice_in_dim(coefficients, block_terms, first_degree, 0)
    initial = jnp.zeros((MODES,) + spectrum.shape[:3], jnp.float32)
    return legendre_sweep(cosines, sines, orders, consume, initial)

def synthesise(scaled, latitudes, orders):
    cosines, sines = colatitude_parts(latitudes)[:2]

    def consume(running, legendre, first_degree):
        scaled_block = lax.dynamic_slice_in_dim(scaled, first_degree, block_degrees, 0)
        return running + jnp.einsum('lmj,lmcf->mcfj', legendre, scaled_block, precision=highest)
    initial = jnp.zeros(scaled.shape[1:] + (latitudes.shape[0],), jnp.float32)
    return legendre_sweep(cosines, sines, orders, consume, initial)

def reference(height, response):
    transform = jnp.fft.rfft(height, axis=2)[:, :, :MODES] * (2.0 * jnp.pi / NLON)
    spectral_parts = jnp.stack([jnp.real(transform), jnp.imag(transform)], axis=0)
    spectral_parts = jnp.transpose(spectral_parts, (3, 0, 1, 2)).astype(jnp.float32)
    all_rows = jnp.arange(NLAT, dtype=jnp.int32)
    groups = spectral_parts.reshape((MODES // block_degrees, block_degrees) + spectral_parts.shape[1:])

    def one_group(group_pair):
        block_index, group_spectrum = group_pair
        orders = block_index * block_degrees + jnp.arange(block_degrees, dtype=jnp.int32)
        coefficients = analyse(group_spectrum, all_rows, orders)
        scaled = coefficients * response[:, None, None, None]
        return synthesise(scaled, all_rows, orders)
    synthesis = lax.map(one_group, (jnp.arange(MODES // block_degrees, dtype=jnp.int32), groups))
    synthesis = synthesis.reshape((MODES,) + synthesis.shape[2:])
    complex_parts = jnp.transpose(synthesis[:, 0] + 1j * synthesis[:, 1], (1, 2, 0))
    padded = jnp.pad(complex_parts, ((0, 0), (0, 0), (0, NLON // 2 + 1 - MODES)))
    loading = jnp.fft.irfft(padded, n=NLON, axis=2) * NLON
    return loading.astype(jnp.float32)
```

```python
import math

import numpy as np
import jax
import jax.numpy as jnp
from jax import lax
from jax.experimental import pallas as pl
from jax.experimental.pallas import tpu as pltpu
from jax.sharding import PartitionSpec as P

NLAT = 1152
NLON = 4096
MODES = 640
LON = 16
LAT = 8
DEVICES = LON * LAT
BAND = NLAT // LAT
CELLS = NLON // LON
SLOTS = MODES // DEVICES
LANES = 128
REST = BAND - LANES
PIECES = 2 * SLOTS
ROWS = PIECES + 2
HALF = LAT // 2
DEPTH = (HALF + 1) * LANES
STEP = 16
BIG = 2.0**60
SMALL = 2.0**-60

f32 = jnp.float32
bf16 = jnp.bfloat16

SLOT_BASE = [sum(MODES - DEVICES * q for q in range(s)) for s in range(SLOTS)]
LEGENDRE_ROWS = sum(MODES - DEVICES * s for s in range(SLOTS))


def split_np(x):
    x = np.asarray(x, np.float32)
    hi = x.astype(jnp.bfloat16)
    lo = (x - hi.astype(np.float32)).astype(jnp.bfloat16)
    return hi, lo


def wave_table():
    m = np.arange(MODES)[:, None]
    r = np.arange(CELLS)[None, :]
    angle = 2.0 * np.pi * ((m * r) % NLON) / NLON
    parts = np.stack([np.cos(angle), -np.sin(angle)]).reshape(2, SLOTS, DEVICES, CELLS)
    return parts.transpose(1, 0, 2, 3).reshape(2 * MODES, CELLS)


def half_rows(values, fill):
    out = np.full((8, LANES), fill, np.float64)
    for y in range(HALF):
        out[y] = values[BAND * y : BAND * y + LANES]
        out[HALF, REST * y : REST * (y + 1)] = values[BAND * y + LANES : BAND * (y + 1)]
    return out


def row_tables():
    theta = np.pi * (np.arange(NLAT // 2) + 0.5) / NLAT
    cosines = half_rows(np.cos(theta), 0.0)
    logs = half_rows(np.log2(np.sin(theta)), 0.0)
    weights = half_rows(np.sin(theta) * np.pi / NLAT * (2.0 * np.pi / NLON), 0.0)
    coarse = np.round(logs * 4096.0) / 4096.0
    coarse = np.where(np.abs(logs) > 2.0, np.round(logs * 1024.0) / 1024.0, coarse)
    starts = [
        0.5 * (math.lgamma(m + 1.5) - math.lgamma(1.5) - math.lgamma(m + 1.0)) - 0.5 * math.log(4.0 * math.pi)
        for m in range(MODES)
    ]
    starts = np.zeros((8, DEVICES)) + np.pad(np.array(starts).reshape(SLOTS, DEVICES), ((0, 3), (0, 0))) / math.log(2.0)
    return np.stack([cosines, coarse, logs - coarse, weights, starts]).astype(np.float32)


def split(x):
    hi = x.astype(bf16)
    return hi, (x - hi.astype(f32)).astype(bf16)


def dot(a, b):
    return lax.dot_general(a, b, (((1,), (0,)), ((), ())), preferred_element_type=f32)


def dot_nt(a, b):
    return lax.dot_general(a, b, (((1,), (1,)), ((), ())), preferred_element_type=f32)


def iota(shape, dim):
    return lax.broadcasted_iota(jnp.int32, shape, dim)


def ones_where(cond):
    return jnp.where(cond, 1.0, 0.0).astype(bf16)


def phases(lon_index):
    turn = (iota((16, LANES), 0) * lon_index) & 15
    angle = turn.astype(f32) * (2.0 * math.pi / 16)
    return (
        jnp.concatenate([jnp.cos(angle)] * 8, axis=0),
        jnp.concatenate([jnp.sin(angle)] * 8, axis=0),
    )


def forward_kernel(h_ref, whi_ref, wlo_ref, o_ref):
    lon_index = lax.axis_index("lon")
    north = lax.axis_index("lat") < HALF
    hi, lo = split(h_ref[0])
    out_row = iota((2 * LANES, BAND), 0)
    in_row = iota((2 * LANES, BAND), 1)
    order = ones_where(in_row == jnp.where(north, out_row, BAND - 1 - out_row))
    hi = dot(order, hi).astype(bf16)
    lo = dot(order, lo).astype(bf16)
    cos, sin = phases(lon_index)
    rest = [jnp.zeros((DEVICES, LANES), f32), jnp.zeros((DEVICES, LANES), f32)]
    for s in range(SLOTS):
        whi = whi_ref[pl.ds(256 * s, 256), :]
        wlo = wlo_ref[pl.ds(256 * s, 256), :]
        terms = dot_nt(whi, hi) + (dot_nt(wlo, hi) + dot_nt(whi, lo))
        for half in range(2):
            real = terms[:DEVICES, LANES * half : LANES * (half + 1)]
            imag = terms[DEVICES:, LANES * half : LANES * (half + 1)]
            turned = (real * cos + imag * sin, imag * cos - real * sin)
            for c in range(2):
                piece = 2 * s + c
                if half == 0:
                    o_ref[pl.ds(piece, DEVICES, stride=ROWS), :] = turned[c]
                else:
                    shift = REST * (piece % 8)
                    moved = pltpu.roll(turned[c], shift, 1) if shift else turned[c]
                    rest[piece // 8] = rest[piece // 8] + moved
    o_ref[pl.ds(PIECES, DEVICES, stride=ROWS), :] = rest[0]
    o_ref[pl.ds(PIECES + 1, DEVICES, stride=ROWS), :] = rest[1]


def legendre_kernel(coef_ref, tab_ref, phi_ref, plo_ref, stage_ref):
    device = lax.axis_index("lon") * LAT + lax.axis_index("lat")
    x = tab_ref[0]
    coarse = tab_ref[1]
    fine = tab_ref[2]
    lane = iota((1, DEVICES), 1)
    firsts, counts = [], []
    for s in range(SLOTS):
        order = (device + DEVICES * s).astype(f32)
        start = jnp.sum(jnp.where(lane == device, tab_ref[4, pl.ds(s, 1), :], 0.0), axis=1, keepdims=True)
        whole = order * coarse
        count = jnp.maximum(jnp.ceil(-whole * (1.0 / 60.0)), 0.0)
        firsts.append(jnp.exp2((whole + 60.0 * count) + (order * fine + start)))
        counts.append(count)
    zero = jnp.zeros((8, LANES), f32)
    state = [(zero, zero, counts[s]) for s in range(SLOTS)]
    for block in range(SLOTS):
        active = block + 1

        def group(g, carried, block=block, active=active):
            carried = list(carried)
            factors = []
            for s in range(active):
                count = carried[3 * s + 2]
                factors.append(
                    jnp.where(
                        count < 0.5,
                        1.0,
                        jnp.where(count < 1.5, SMALL, jnp.where(count < 2.5, SMALL * SMALL, 0.0)),
                    )
                )
            for n in range(STEP):
                degree = block * DEVICES + g * STEP + n
                for s in range(active):
                    earlier, latest = carried[3 * s], carried[3 * s + 1]
                    growth = coef_ref[s * MODES + degree]
                    damped = coef_ref[(SLOTS + s) * MODES + degree]
                    current = (growth * x) * latest - damped * earlier
                    if s == block:
                        current = jnp.where(degree == device + DEVICES * s, firsts[s], current)
                    row = s * DEVICES * 8 + (g * STEP + n) * 8
                    stage_ref[pl.ds(pl.multiple_of(row, 8), 8), :] = current * factors[s]
                    carried[3 * s], carried[3 * s + 1] = latest, current
            for s in range(active):
                earlier, latest, count = carried[3 * s : 3 * s + 3]
                largest = jnp.maximum(jnp.abs(earlier), jnp.abs(latest))
                large = jnp.logical_and(largest > BIG, count > 0.5)
                scale = jnp.where(large, SMALL, 1.0)
                carried[3 * s] = earlier * scale
                carried[3 * s + 1] = latest * scale
                carried[3 * s + 2] = count - jnp.where(large, 1.0, 0.0)
            return tuple(carried)

        flat = tuple(v for s in range(active) for v in state[s])
        flat = lax.fori_loop(0, DEVICES // STEP, group, flat)
        for s in range(active):
            state[s] = flat[3 * s : 3 * s + 3]
            first = SLOT_BASE[s] + (block - s) * DEVICES
            for b in range(HALF + 1):
                piece = stage_ref[pl.ds(s * DEVICES * 8 + b, DEVICES, stride=8), :]
                hi, lo = split(piece)
                phi_ref[pl.ds(first, DEVICES), LANES * b : LANES * (b + 1)] = hi
                plo_ref[pl.ds(first, DEVICES), LANES * b : LANES * (b + 1)] = lo


def degree_kernel(t_ref, phi_ref, plo_ref, tab_ref, resp_ref, o_ref, sum_ref, fold_ref, rest_ref, back_ref):
    device = lax.axis_index("lon") * LAT + lax.axis_index("lat")
    block = LAT * ROWS
    total = t_ref[pl.ds(0, block), :]
    for i in range(1, LON):
        total = total + t_ref[pl.ds(block * i, block), :]
    sum_ref[...] = total
    fold_ref[...] = jnp.zeros(fold_ref.shape, f32)
    piece = iota((16, LANES), 0)
    own = jnp.logical_and((iota((16, LANES), 1) // REST) == piece % 8, piece < PIECES)
    for y in range(HALF):
        upper = sum_ref[pl.ds(ROWS * y, ROWS), :]
        lower = sum_ref[pl.ds(ROWS * (LAT - 1 - y), ROWS), :]
        for p, folded in enumerate((upper + lower, upper - lower)):
            fold_ref[pl.ds(16 * p, ROWS), LANES * y : LANES * (y + 1)] = folded * tab_ref[3, pl.ds(y, 1), :]
            spread = jnp.where(piece < 8, folded[PIECES : PIECES + 1], folded[PIECES + 1 : PIECES + 2])
            rest_ref[pl.ds(16 * p, 16), LANES * y : LANES * (y + 1)] = jnp.where(own, spread, 0.0)
    lane_in = iota((HALF * LANES, LANES), 0)
    lane_out = iota((HALF * LANES, LANES), 1)
    place = ones_where(
        jnp.logical_and(lane_in % REST == lane_out % REST, lane_in // LANES == lane_out // REST)
    )
    rest_hi, rest_lo = split(rest_ref[...])
    rest = dot(rest_hi, place) + dot(rest_lo, place)
    fold_ref[:, DEPTH - LANES :] = rest * tab_ref[3, pl.ds(HALF, 1), :]
    fold_hi, fold_lo = split(fold_ref[...])
    both = jnp.concatenate([fold_hi, fold_lo], axis=0)
    back_ref[...] = jnp.zeros(back_ref.shape, f32)
    for s in range(SLOTS):
        count = MODES - DEVICES * s
        rows = pl.ds(SLOT_BASE[s], count)
        phi = phi_ref[rows, :]
        plo = plo_ref[rows, :]
        main = dot_nt(both, phi)
        terms = main[:32] + (main[32:] + dot_nt(fold_hi, plo))
        even = ((iota((2, count), 1) + device) & 1) == 0
        chosen = jnp.where(even, terms[2 * s : 2 * s + 2], terms[16 + 2 * s : 18 + 2 * s])
        weight = 2.0 if s else jnp.where(device == 0, 1.0, 2.0)
        scaled = chosen * (resp_ref[:, DEVICES * s :] * weight)
        four = jnp.concatenate(
            [jnp.where(even, scaled, 0.0), jnp.where(even, 0.0, scaled), jnp.zeros((4, count), f32)], axis=0
        )
        hi, lo = split(four)
        pair = jnp.concatenate([hi, lo], axis=0)
        out = dot(pair, phi)
        sums = out[:8] + (out[8:] + dot(hi, plo))
        back_ref[pl.ds(2 * s, 2), :] = sums[0:2] + sums[2:4]
        back_ref[pl.ds(16 + 2 * s, 2), :] = sums[0:2] - sums[2:4]
    pick_in = iota((LANES, HALF * LANES), 0)
    pick_out = iota((LANES, HALF * LANES), 1)
    pick = ones_where(
        jnp.logical_and(pick_in % REST == pick_out % REST, pick_in // REST == pick_out // LANES)
    )
    rest_hi, rest_lo = split(back_ref[:, DEPTH - LANES :])
    rest = dot(rest_hi, pick) + dot(rest_lo, pick)
    for p in range(2):
        for y in range(HALF):
            band = y if p == 0 else LAT - 1 - y
            sum_ref[pl.ds(ROWS * band, PIECES), :] = back_ref[pl.ds(16 * p, PIECES), LANES * y : LANES * (y + 1)]
            kept = jnp.where(own, rest[16 * p : 16 * (p + 1), LANES * y : LANES * (y + 1)], 0.0)
            sum_ref[pl.ds(ROWS * band + PIECES, 1), :] = jnp.sum(kept[:8], axis=0, keepdims=True)
            sum_ref[pl.ds(ROWS * band + PIECES + 1, 1), :] = jnp.sum(kept[8:], axis=0, keepdims=True)
    total = sum_ref[...]
    for i in range(LON):
        o_ref[pl.ds(block * i, block), :] = total


def inverse_kernel(r_ref, whi_ref, wlo_ref, o_ref):
    lon_index = lax.axis_index("lon")
    north = lax.axis_index("lat") < HALF
    cos, sin = phases(lon_index)
    rest = [
        r_ref[pl.ds(PIECES, DEVICES, stride=ROWS), :],
        r_ref[pl.ds(PIECES + 1, DEVICES, stride=ROWS), :],
    ]
    valid = iota((DEVICES, LANES), 1) < REST
    total = None
    for s in range(SLOTS):
        halves = []
        for half in range(2):
            parts = []
            for c in range(2):
                piece = 2 * s + c
                if half == 0:
                    parts.append(r_ref[pl.ds(piece, DEVICES, stride=ROWS), :])
                else:
                    shift = (LANES - REST * (piece % 8)) % LANES
                    moved = pltpu.roll(rest[piece // 8], shift, 1) if shift else rest[piece // 8]
                    parts.append(jnp.where(valid, moved, 0.0))
            real, imag = parts
            halves.append(jnp.concatenate([real * cos - imag * sin, real * sin + imag * cos], axis=0))
        hi, lo = split(jnp.concatenate(halves, axis=1))
        whi = whi_ref[:, 256 * s : 256 * (s + 1)]
        wlo = wlo_ref[:, 256 * s : 256 * (s + 1)]
        terms = dot(whi, hi) + (dot(wlo, hi) + dot(whi, lo))
        total = terms if total is None else total + terms
    out_row = iota((BAND, 2 * LANES), 0)
    in_row = iota((BAND, 2 * LANES), 1)
    order = ones_where(in_row == jnp.where(north, out_row, BAND - 1 - out_row))
    first, rest_of = split(total)
    second, third = split(total - first.astype(f32))
    o_ref[0] = dot_nt(order, first) + (dot_nt(order, second) + dot_nt(order, third))


def vmem(n):
    return [pl.BlockSpec(memory_space=pltpu.VMEM)] * n


def exchanged(x):
    x = x.reshape(DEVICES, 1, ROWS * LANES)
    x = lax.all_to_all(x, ("lon", "lat"), split_axis=0, concat_axis=0, tiled=True)
    return x.reshape(DEVICES * ROWS, LANES)


def recurrence_factors(device):
    degree = jnp.arange(MODES, dtype=jnp.int32)[None, :]
    order = (device + DEVICES * jnp.arange(SLOTS, dtype=jnp.int32))[:, None]
    started = degree > order
    l = degree.astype(f32)
    m = order.astype(f32)
    k = l - 1.0
    growth = jnp.where(started, jnp.sqrt((4.0 * l * l - 1.0) / jnp.where(started, l * l - m * m, 1.0)), 0.0)
    damping = jnp.sqrt(jnp.where(started, k * k - m * m, 0.0) / jnp.maximum(4.0 * k * k - 1.0, 1.0))
    return jnp.stack([growth, growth * damping]).reshape(2 * SLOTS * MODES)


def shards(height, response):
    device = lax.axis_index("lon") * LAT + lax.axis_index("lat")
    table = wave_table()
    whi, wlo = split_np(table)
    thi, tlo = split_np(table.T)
    tables = jnp.asarray(row_tables())
    packed = jax.ShapeDtypeStruct((DEVICES * ROWS, LANES), f32)
    shares = pl.pallas_call(
        forward_kernel, out_shape=packed, in_specs=vmem(3), out_specs=vmem(1)[0], name="forward_dft"
    )(height, jnp.asarray(whi), jnp.asarray(wlo))
    legendre = jax.ShapeDtypeStruct((LEGENDRE_ROWS, DEPTH), bf16)
    phi, plo = pl.pallas_call(
        legendre_kernel,
        out_shape=(legendre, legendre),
        in_specs=[pl.BlockSpec(memory_space=pltpu.SMEM)] + vmem(1),
        out_specs=tuple(vmem(2)),
        scratch_shapes=[pltpu.VMEM((SLOTS * DEVICES * 8, LANES), f32)],
        name="legendre",
    )(recurrence_factors(device), tables)
    arrived = exchanged(shares)
    synthesis = pl.pallas_call(
        degree_kernel,
        out_shape=packed,
        in_specs=vmem(5),
        out_specs=vmem(1)[0],
        scratch_shapes=[
            pltpu.VMEM((LAT * ROWS, LANES), f32),
            pltpu.VMEM((32, DEPTH), f32),
            pltpu.VMEM((32, HALF * LANES), f32),
            pltpu.VMEM((32, DEPTH), f32),
        ],
        name="degrees",
    )(arrived, phi, plo, tables, response.reshape(1, MODES))
    returned = exchanged(synthesis)
    return pl.pallas_call(
        inverse_kernel,
        out_shape=jax.ShapeDtypeStruct((1, BAND, CELLS), f32),
        in_specs=vmem(3),
        out_specs=vmem(1)[0],
        name="inverse_dft",
    )(returned, jnp.asarray(thi), jnp.asarray(tlo))


def solution(mesh):
    placed = (P(None, "lat", "lon"), P())
    return jax.shard_map(
        shards, mesh=mesh, in_specs=placed, out_specs=P(None, "lat", "lon"), check_vma=False
    )
```

```python
import math

import numpy as np
import jax
import jax.numpy as jnp
from jax import lax
from jax.experimental import pallas as pl
from jax.experimental.pallas import tpu as pltpu
from jax.sharding import PartitionSpec as P

NLAT = 1152
NLON = 4096
MODES = 640
LON = 16
LAT = 8
DEVICES = LON * LAT
BAND = NLAT // LAT
CELLS = NLON // LON
SLOTS = MODES // DEVICES
LANES = 128
PART = BAND // 2
MAIN = 64
REST = PART - MAIN
ROWS = SLOTS + 1
PAIRS = LON // 2
HALF = LAT // 2
DEPTH = (HALF + 1) * LANES
STEP = 16
LEGENDRE_FIRST = False
BIG = 2.0**60
SMALL = 2.0**-60

f32 = jnp.float32
bf16 = jnp.bfloat16

SLOT_BASE = [sum(MODES - DEVICES * q for q in range(s)) for s in range(SLOTS)]
LEGENDRE_ROWS = sum(MODES - DEVICES * s for s in range(SLOTS))


def split_np(x):
    x = np.asarray(x, np.float32)
    hi = x.astype(jnp.bfloat16)
    lo = (x - hi.astype(np.float32)).astype(jnp.bfloat16)
    return hi, lo


def wave_table():
    m = np.arange(MODES)[:, None]
    r = np.arange(CELLS)[None, :]
    angle = 2.0 * np.pi * ((m * r) % NLON) / NLON
    parts = np.stack([np.cos(angle), -np.sin(angle)]).reshape(2, SLOTS, DEVICES, CELLS)
    return parts.transpose(1, 0, 2, 3).reshape(2 * MODES, CELLS)


def half_rows(values, fill):
    out = np.full((8, LANES), fill, np.float64)
    for y in range(HALF):
        for c in range(2):
            part = values[BAND * y + PART * c : BAND * y + PART * (c + 1)]
            out[y, MAIN * c : MAIN * (c + 1)] = part[:MAIN]
            first = REST * (2 * y + c)
            out[HALF, first : first + REST] = part[MAIN:]
    return out


def row_tables():
    theta = np.pi * (np.arange(NLAT // 2) + 0.5) / NLAT
    cosines = half_rows(np.cos(theta), 0.0)
    logs = half_rows(np.log2(np.sin(theta)), 0.0)
    weights = half_rows(np.sin(theta) * np.pi / NLAT * (2.0 * np.pi / NLON), 0.0)
    coarse = np.round(logs * 4096.0) / 4096.0
    coarse = np.where(np.abs(logs) > 2.0, np.round(logs * 1024.0) / 1024.0, coarse)
    starts = [
        0.5 * (math.lgamma(m + 1.5) - math.lgamma(1.5) - math.lgamma(m + 1.0)) - 0.5 * math.log(4.0 * math.pi)
        for m in range(MODES)
    ]
    starts = np.zeros((8, DEVICES)) + np.pad(np.array(starts).reshape(SLOTS, DEVICES), ((0, 3), (0, 0))) / math.log(2.0)
    return np.stack([cosines, coarse, logs - coarse, weights, starts]).astype(np.float32)


def split(x):
    hi = x.astype(bf16)
    return hi, (x - hi.astype(f32)).astype(bf16)


def dot(a, b):
    return lax.dot_general(a, b, (((1,), (0,)), ((), ())), preferred_element_type=f32)


def dot_nt(a, b):
    return lax.dot_general(a, b, (((1,), (1,)), ((), ())), preferred_element_type=f32)


def iota(shape, dim):
    return lax.broadcasted_iota(jnp.int32, shape, dim)


def ones_where(cond):
    return jnp.where(cond, 1.0, 0.0).astype(bf16)


def phases(lon_index):
    turn = (iota((16, LANES), 0) * lon_index) & 15
    angle = turn.astype(f32) * (2.0 * math.pi / 16)
    return (
        jnp.concatenate([jnp.cos(angle)] * 8, axis=0),
        jnp.concatenate([jnp.sin(angle)] * 8, axis=0),
    )


def turned_back(terms, cos, sin):
    real, imag = terms[:DEVICES], terms[DEVICES:]
    return real * cos + imag * sin, imag * cos - real * sin


def forward_kernel(h_ref, g_ref, whi_ref, wlo_ref, o_ref):
    lon_index = lax.axis_index("lon")
    part = lon_index & 1
    north = lax.axis_index("lat") < HALF
    own_hi, own_lo = split(h_ref[0])
    got_hi, got_lo = split(g_ref[0])
    out_row = iota((LANES, BAND), 0)
    place = PART * part + out_row
    source = jnp.where(north, place, BAND - 1 - place)
    own = ones_where(jnp.logical_and(iota((LANES, BAND), 1) == source, out_row < PART))
    out_row = iota((LANES, PART), 0)
    source = jnp.where(north, out_row, PART - 1 - out_row)
    got = ones_where(jnp.logical_and(iota((LANES, PART), 1) == source, out_row < PART))
    hi = jnp.concatenate([dot(own, own_hi), dot(got, got_hi)], axis=0).astype(bf16)
    lo = jnp.concatenate([dot(own, own_lo), dot(got, got_lo)], axis=0).astype(bf16)
    own_cos, own_sin = phases(lon_index)
    got_cos, got_sin = phases(lon_index ^ 1)
    lane = iota((DEVICES, LANES), 1)
    is_rest = lane // REST == MAIN // REST
    rest = jnp.zeros((DEVICES, LANES), f32)
    for s in range(SLOTS):
        whi = whi_ref[pl.ds(256 * s, 256), :]
        wlo = wlo_ref[pl.ds(256 * s, 256), :]
        terms = dot_nt(whi, hi) + (dot_nt(wlo, hi) + dot_nt(whi, lo))
        own_real, own_imag = turned_back(terms[:, :LANES], own_cos, own_sin)
        got_real, got_imag = turned_back(terms[:, LANES:], got_cos, got_sin)
        real, imag = own_real + got_real, own_imag + got_imag
        o_ref[pl.ds(s, DEVICES, stride=ROWS), :] = jnp.where(lane < MAIN, real, pltpu.roll(imag, MAIN, 1))
        for c, value in enumerate((real, imag)):
            shift = (REST * (s + 8 * c) - MAIN) % LANES
            kept = jnp.where(is_rest, value, 0.0)
            rest = rest + (pltpu.roll(kept, shift, 1) if shift else kept)
    o_ref[pl.ds(SLOTS, DEVICES, stride=ROWS), :] = rest


def legendre_kernel(coef_ref, tab_ref, phi_ref, plo_ref, stage_ref):
    device = lax.axis_index("lon") * LAT + lax.axis_index("lat")
    x = tab_ref[0]
    coarse = tab_ref[1]
    fine = tab_ref[2]
    lane = iota((1, DEVICES), 1)
    firsts, counts = [], []
    for s in range(SLOTS):
        order = (device + DEVICES * s).astype(f32)
        start = jnp.sum(jnp.where(lane == device, tab_ref[4, pl.ds(s, 1), :], 0.0), axis=1, keepdims=True)
        whole = order * coarse
        count = jnp.maximum(jnp.ceil(-whole * (1.0 / 60.0)), 0.0)
        firsts.append(jnp.exp2((whole + 60.0 * count) + (order * fine + start)))
        counts.append(count)
    zero = jnp.zeros((8, LANES), f32)
    state = [(zero, zero, counts[s]) for s in range(SLOTS)]
    for block in range(SLOTS):
        active = block + 1

        def group(g, carried, block=block, active=active):
            carried = list(carried)
            factors = []
            for s in range(active):
                count = carried[3 * s + 2]
                factors.append(
                    jnp.where(
                        count < 0.5,
                        1.0,
                        jnp.where(count < 1.5, SMALL, jnp.where(count < 2.5, SMALL * SMALL, 0.0)),
                    )
                )
            for n in range(STEP):
                degree = block * DEVICES + g * STEP + n
                for s in range(active):
                    earlier, latest = carried[3 * s], carried[3 * s + 1]
                    growth = coef_ref[s * MODES + degree]
                    damped = coef_ref[(SLOTS + s) * MODES + degree]
                    current = (growth * x) * latest - damped * earlier
                    if s == block:
                        current = jnp.where(degree == device + DEVICES * s, firsts[s], current)
                    row = s * DEVICES * 8 + (g * STEP + n) * 8
                    stage_ref[pl.ds(pl.multiple_of(row, 8), 8), :] = current * factors[s]
                    carried[3 * s], carried[3 * s + 1] = latest, current
            for s in range(active):
                earlier, latest, count = carried[3 * s : 3 * s + 3]
                largest = jnp.maximum(jnp.abs(earlier), jnp.abs(latest))
                large = jnp.logical_and(largest > BIG, count > 0.5)
                scale = jnp.where(large, SMALL, 1.0)
                carried[3 * s] = earlier * scale
                carried[3 * s + 1] = latest * scale
                carried[3 * s + 2] = count - jnp.where(large, 1.0, 0.0)
            return tuple(carried)

        flat = tuple(v for s in range(active) for v in state[s])
        flat = lax.fori_loop(0, DEVICES // STEP, group, flat)
        for s in range(active):
            state[s] = flat[3 * s : 3 * s + 3]
            first = SLOT_BASE[s] + (block - s) * DEVICES
            for b in range(HALF + 1):
                piece = stage_ref[pl.ds(s * DEVICES * 8 + b, DEVICES, stride=8), :]
                hi, lo = split(piece)
                phi_ref[pl.ds(first, DEVICES), LANES * b : LANES * (b + 1)] = hi
                plo_ref[pl.ds(first, DEVICES), LANES * b : LANES * (b + 1)] = lo


def degree_kernel(t_ref, phi_ref, plo_ref, tab_ref, resp_ref, o_ref, sum_ref, fold_ref, rest_ref, back_ref):
    device = lax.axis_index("lon") * LAT + lax.axis_index("lat")
    block = LAT * ROWS
    for c in range(2):
        total = t_ref[pl.ds(block * c, block), :]
        for i in range(1, PAIRS):
            total = total + t_ref[pl.ds(block * (2 * i + c), block), :]
        sum_ref[pl.ds(block * c, block), :] = total
    fold_ref[...] = jnp.zeros(fold_ref.shape, f32)
    own = iota((16, LANES), 1) // REST == iota((16, LANES), 0)
    first = iota((ROWS, LANES), 1) < MAIN
    for y in range(HALF):
        mains = []
        for c in range(2):
            upper = sum_ref[pl.ds(block * c + ROWS * y, ROWS), :]
            lower = sum_ref[pl.ds(block * c + ROWS * (LAT - 1 - y), ROWS), :]
            mains.append((upper + lower, upper - lower))
        lanes = slice(LANES * y, LANES * (y + 1))
        for p in range(2):
            left, right = mains[0][p], mains[1][p]
            weight = tab_ref[3, pl.ds(y, 1), :]
            fold_ref[pl.ds(16 * p, ROWS), lanes] = jnp.where(first, left, pltpu.roll(right, MAIN, 1)) * weight
            fold_ref[pl.ds(16 * p + 8, ROWS), lanes] = jnp.where(first, pltpu.roll(left, MAIN, 1), right) * weight
            for c in range(2):
                spread = jnp.where(own, mains[c][p][SLOTS : SLOTS + 1], 0.0)
                group = 2 * y + c
                rest_ref[pl.ds(16 * p, 16), LANES * group : LANES * (group + 1)] = spread
    lane_in = iota((LAT * LANES, LANES), 0)
    lane_out = iota((LAT * LANES, LANES), 1)
    place = ones_where(
        jnp.logical_and(lane_in % REST == lane_out % REST, lane_in // LANES == lane_out // REST)
    )
    rest_hi, rest_lo = split(rest_ref[...])
    rest = dot(rest_hi, place) + dot(rest_lo, place)
    fold_ref[:, DEPTH - LANES :] = rest * tab_ref[3, pl.ds(HALF, 1), :]
    fold_hi, fold_lo = split(fold_ref[...])
    both = jnp.concatenate([fold_hi, fold_lo], axis=0)
    back_ref[...] = jnp.zeros(back_ref.shape, f32)
    for s in range(SLOTS):
        count = MODES - DEVICES * s
        rows = pl.ds(SLOT_BASE[s], count)
        phi = phi_ref[rows, :]
        plo = plo_ref[rows, :]
        main = dot_nt(both, phi)
        terms = main[:32] + (main[32:] + dot_nt(fold_hi, plo))
        degree = iota((1, count), 1)
        even = ((degree + device) & 1) == 0
        weight = 2.0 if s else jnp.where(device == 0, 1.0, 2.0)
        factor = resp_ref[:, DEVICES * s :] * weight
        real = jnp.where(even, terms[s : s + 1], terms[16 + s : 17 + s]) * factor
        imag = jnp.where(even, terms[8 + s : 9 + s], terms[24 + s : 25 + s]) * factor
        four = jnp.concatenate(
            [
                jnp.where(even, real, 0.0),
                jnp.where(even, imag, 0.0),
                jnp.where(even, 0.0, real),
                jnp.where(even, 0.0, imag),
                jnp.zeros((4, count), f32),
            ],
            axis=0,
        )
        hi, lo = split(four)
        out = dot(jnp.concatenate([hi, lo], axis=0), phi)
        sums = out[:8] + (out[8:] + dot(hi, plo))
        for c in range(2):
            back_ref[pl.ds(8 * c + s, 1), :] = sums[c : c + 1] + sums[2 + c : 3 + c]
            back_ref[pl.ds(16 + 8 * c + s, 1), :] = sums[c : c + 1] - sums[2 + c : 3 + c]
    pick_in = iota((LANES, LAT * LANES), 0)
    pick_out = iota((LANES, LAT * LANES), 1)
    pick = ones_where(
        jnp.logical_and(pick_in % REST == pick_out % REST, pick_in // REST == pick_out // LANES)
    )
    rest_hi, rest_lo = split(back_ref[:, DEPTH - LANES :])
    rest = dot(rest_hi, pick) + dot(rest_lo, pick)
    for p in range(2):
        for y in range(HALF):
            band = y if p == 0 else LAT - 1 - y
            lanes = slice(LANES * y, LANES * (y + 1))
            real = back_ref[pl.ds(16 * p, ROWS), lanes]
            imag = back_ref[pl.ds(16 * p + 8, ROWS), lanes]
            for c in range(2):
                row = block * c + ROWS * band
                if c == 0:
                    sum_ref[pl.ds(row, ROWS), :] = jnp.where(first, real, pltpu.roll(imag, MAIN, 1))
                else:
                    sum_ref[pl.ds(row, ROWS), :] = jnp.where(first, pltpu.roll(real, MAIN, 1), imag)
                group = 2 * y + c
                kept = jnp.where(own, rest[16 * p : 16 * (p + 1), LANES * group : LANES * (group + 1)], 0.0)
                sum_ref[pl.ds(row + SLOTS, 1), :] = jnp.sum(kept, axis=0, keepdims=True)
    for c in range(2):
        total = sum_ref[pl.ds(block * c, block), :]
        for i in range(PAIRS):
            o_ref[pl.ds(block * (2 * i + c), block), :] = total


def inverse_kernel(r_ref, g_ref, whi_ref, wlo_ref, o_ref):
    lon_index = lax.axis_index("lon")
    part = lon_index & 1
    north = lax.axis_index("lat") < HALF
    cos, sin = phases(lon_index)
    lane = iota((DEVICES, LANES), 1)
    is_main = lane < MAIN
    is_rest = lane // REST == MAIN // REST
    total = None
    for s in range(SLOTS):
        halves = []
        for ref in (r_ref, g_ref):
            main = ref[pl.ds(s, DEVICES, stride=ROWS), :]
            rest = ref[pl.ds(SLOTS, DEVICES, stride=ROWS), :]
            parts = []
            for c in range(2):
                shift = (MAIN - REST * (s + 8 * c)) % LANES
                moved = pltpu.roll(rest, shift, 1) if shift else rest
                body = pltpu.roll(main, MAIN, 1) if c else main
                parts.append(jnp.where(is_main, body, jnp.where(is_rest, moved, 0.0)))
            real, imag = parts
            halves.append(jnp.concatenate([real * cos - imag * sin, real * sin + imag * cos], axis=0))
        hi, lo = split(jnp.concatenate(halves, axis=1))
        whi = whi_ref[:, 256 * s : 256 * (s + 1)]
        wlo = wlo_ref[:, 256 * s : 256 * (s + 1)]
        terms = dot(whi, hi) + (dot(wlo, hi) + dot(whi, lo))
        total = terms if total is None else total + terms
    row = iota((BAND, 2 * LANES), 0)
    place = jnp.where(north, row, BAND - 1 - row) - PART * part
    mine = jnp.logical_and(place >= 0, place < PART)
    other = jnp.where(place < 0, place + PART, place - PART) + LANES
    order = ones_where(iota((BAND, 2 * LANES), 1) == jnp.where(mine, place, other))
    first, rest_of = split(total)
    second, third = split(total - first.astype(f32))
    o_ref[0] = dot_nt(order, first) + (dot_nt(order, second) + dot_nt(order, third))


def vmem(n):
    return [pl.BlockSpec(memory_space=pltpu.VMEM)] * n


def limit(mib):
    return pltpu.CompilerParams(vmem_limit_bytes=mib * 2**20)


def swapped(x):
    return lax.ppermute(x, "lon", [(i, i ^ 1) for i in range(LON)])


def exchanged(x):
    x = x.reshape(DEVICES, 1, ROWS * LANES)
    x = lax.all_to_all(x, ("lon", "lat"), split_axis=0, concat_axis=0, tiled=True)
    return x.reshape(DEVICES * ROWS, LANES)


def recurrence_factors(device):
    degree = jnp.arange(MODES, dtype=jnp.int32)[None, :]
    order = (device + DEVICES * jnp.arange(SLOTS, dtype=jnp.int32))[:, None]
    started = degree > order
    l = degree.astype(f32)
    m = order.astype(f32)
    k = l - 1.0
    growth = jnp.where(started, jnp.sqrt((4.0 * l * l - 1.0) / jnp.where(started, l * l - m * m, 1.0)), 0.0)
    damping = jnp.sqrt(jnp.where(started, k * k - m * m, 0.0) / jnp.maximum(4.0 * k * k - 1.0, 1.0))
    return jnp.stack([growth, growth * damping]).reshape(2 * SLOTS * MODES)


def shards(height, response):
    device = lax.axis_index("lon") * LAT + lax.axis_index("lat")
    table = wave_table()
    whi, wlo = split_np(table)
    thi, tlo = split_np(table.T)
    tables = jnp.asarray(row_tables())
    packed = jax.ShapeDtypeStruct((DEVICES * ROWS, LANES), f32)
    north = lax.axis_index("lat") < HALF
    part = lax.axis_index("lon") & 1
    start = jnp.where(north, PART * (1 - part), PART * part)
    got = swapped(lax.dynamic_slice_in_dim(height, start, PART, 1))
    legendre = jax.ShapeDtypeStruct((LEGENDRE_ROWS, DEPTH), bf16)
    phi, plo = pl.pallas_call(
        legendre_kernel,
        out_shape=(legendre, legendre),
        in_specs=[pl.BlockSpec(memory_space=pltpu.SMEM)] + vmem(1),
        out_specs=tuple(vmem(2)),
        scratch_shapes=[pltpu.VMEM((SLOTS * DEVICES * 8, LANES), f32)],
        compiler_params=limit(16),
        name="legendre",
    )(recurrence_factors(device), tables)
    if LEGENDRE_FIRST:
        height, got, phi, plo = lax.optimization_barrier((height, got, phi, plo))
    shares = pl.pallas_call(
        forward_kernel,
        out_shape=packed,
        in_specs=vmem(4),
        out_specs=vmem(1)[0],
        compiler_params=limit(12),
        name="forward_dft",
    )(height, got, jnp.asarray(whi), jnp.asarray(wlo))
    arrived = exchanged(shares)
    synthesis = pl.pallas_call(
        degree_kernel,
        out_shape=packed,
        in_specs=vmem(5),
        out_specs=vmem(1)[0],
        scratch_shapes=[
            pltpu.VMEM((2 * LAT * ROWS, LANES), f32),
            pltpu.VMEM((32, DEPTH), f32),
            pltpu.VMEM((32, LAT * LANES), f32),
            pltpu.VMEM((32, DEPTH), f32),
        ],
        compiler_params=limit(16),
        name="degrees",
    )(arrived, phi, plo, tables, response.reshape(1, MODES))
    returned = exchanged(synthesis)
    return pl.pallas_call(
        inverse_kernel,
        out_shape=jax.ShapeDtypeStruct((1, BAND, CELLS), f32),
        in_specs=vmem(4),
        out_specs=vmem(1)[0],
        compiler_params=limit(12),
        name="inverse_dft",
    )(returned, swapped(returned), jnp.asarray(thi), jnp.asarray(tlo))


def solution(mesh):
    placed = (P(None, "lat", "lon"), P())
    return jax.shard_map(
        shards, mesh=mesh, in_specs=placed, out_specs=P(None, "lat", "lon"), check_vma=False
    )
```

```python
import math

import numpy as np
import jax
import jax.numpy as jnp
from jax import lax
from jax.experimental import pallas as pl
from jax.experimental.pallas import tpu as pltpu
from jax.sharding import PartitionSpec as P

NLAT = 1152
NLON = 4096
MODES = 640
LON = 16
LAT = 8
DEVICES = LON * LAT
BAND = NLAT // LAT
CELLS = NLON // LON
SLOTS = MODES // DEVICES
LANES = 128
PART = BAND // 2
MAIN = 64
REST = PART - MAIN
ROWS = SLOTS + 1
PAIRS = LON // 2
HALF = LAT // 2
DEPTH = (HALF + 1) * LANES
STEP = 16
TURN = NLON // DEVICES
BIG = 2.0**60
SMALL = 2.0**-60

f32 = jnp.float32
bf16 = jnp.bfloat16

KEPT = (0, 2)
SENT = tuple(s for s in range(SLOTS) if s not in KEPT)
DEGREES = [MODES - DEVICES * s for s in range(SLOTS)]
SLOT_BASE = [sum(DEGREES[q] for q in (KEPT if s in KEPT else SENT) if q < s) for s in range(SLOTS)]
KEPT_ROWS = sum(DEGREES[s] for s in KEPT)
SENT_ROWS = sum(DEGREES[s] for s in SENT)


def split_np(x):
    x = np.asarray(x, np.float32)
    hi = x.astype(jnp.bfloat16)
    lo = (x - hi.astype(np.float32)).astype(jnp.bfloat16)
    return hi, lo


def wave_table():
    m = np.arange(MODES)[:, None]
    r = np.arange(CELLS)[None, :]
    angle = 2.0 * np.pi * ((m * r) % NLON) / NLON
    parts = np.stack([np.cos(angle), -np.sin(angle)]).reshape(2, SLOTS, DEVICES, CELLS)
    return parts.transpose(1, 0, 2, 3).reshape(2 * MODES, CELLS)


def first_waves(table):
    turns = 2.0 * np.pi * np.arange(8)[:, None] * np.arange(CELLS)[None, :] / TURN
    turns = np.stack([np.cos(turns), np.sin(turns)], axis=1).reshape(16, CELLS)
    return np.concatenate([table[: 2 * DEVICES], turns]).astype(np.float32)


def last_waves(table):
    turns = 2.0 * np.pi * np.arange(SLOTS)[:, None] * np.arange(TURN)[None, :] / TURN
    turns = np.stack([np.cos(turns), np.sin(turns)], axis=1).reshape(2 * SLOTS * TURN, 1)
    turns = np.broadcast_to(turns, (2 * SLOTS * TURN, LANES))
    return table[: 2 * DEVICES].T.astype(np.float32), turns.astype(np.float32)


def half_rows(values, fill):
    out = np.full((8, LANES), fill, np.float64)
    for y in range(HALF):
        for c in range(2):
            part = values[BAND * y + PART * c : BAND * y + PART * (c + 1)]
            out[y, MAIN * c : MAIN * (c + 1)] = part[:MAIN]
            first = REST * (2 * y + c)
            out[HALF, first : first + REST] = part[MAIN:]
    return out


def row_tables():
    theta = np.pi * (np.arange(NLAT // 2) + 0.5) / NLAT
    cosines = half_rows(np.cos(theta), 0.0)
    logs = half_rows(np.log2(np.sin(theta)), 0.0)
    weights = half_rows(np.sin(theta) * np.pi / NLAT * (2.0 * np.pi / NLON), 0.0)
    coarse = np.round(logs * 4096.0) / 4096.0
    coarse = np.where(np.abs(logs) > 2.0, np.round(logs * 1024.0) / 1024.0, coarse)
    starts = [
        0.5 * (math.lgamma(m + 1.5) - math.lgamma(1.5) - math.lgamma(m + 1.0)) - 0.5 * math.log(4.0 * math.pi)
        for m in range(MODES)
    ]
    starts = np.zeros((8, DEVICES)) + np.pad(np.array(starts).reshape(SLOTS, DEVICES), ((0, 3), (0, 0))) / math.log(2.0)
    return np.stack([cosines, coarse, logs - coarse, weights, starts]).astype(np.float32)


def split(x):
    hi = x.astype(bf16)
    return hi, (x - hi.astype(f32)).astype(bf16)


def dot(a, b):
    return lax.dot_general(a, b, (((1,), (0,)), ((), ())), preferred_element_type=f32)


def dot_nt(a, b):
    return lax.dot_general(a, b, (((1,), (1,)), ((), ())), preferred_element_type=f32)


def iota(shape, dim):
    return lax.broadcasted_iota(jnp.int32, shape, dim)


def ones_where(cond):
    return jnp.where(cond, 1.0, 0.0).astype(bf16)


def phases(lon_index):
    turn = (iota((16, LANES), 0) * lon_index) & 15
    angle = turn.astype(f32) * (2.0 * math.pi / 16)
    return (
        jnp.concatenate([jnp.cos(angle)] * 8, axis=0),
        jnp.concatenate([jnp.sin(angle)] * 8, axis=0),
    )


def turned_back(terms, cos, sin):
    real, imag = terms[:DEVICES], terms[DEVICES:]
    return real * cos + imag * sin, imag * cos - real * sin


def band_order():
    part = lax.axis_index("lon") & 1
    north = lax.axis_index("lat") < HALF
    out_row = iota((LANES, BAND), 0)
    place = PART * part + out_row
    source = jnp.where(north, place, BAND - 1 - place)
    return ones_where(jnp.logical_and(iota((LANES, BAND), 1) == source, out_row < PART))


def own_kernel(h_hbm, wave_hbm, hi_ref, lo_ref, whi_ref, wlo_ref, h_ref, wave_ref, sems):
    copies = (
        pltpu.make_async_copy(wave_hbm, wave_ref, sems.at[0]),
        pltpu.make_async_copy(h_hbm, h_ref, sems.at[1]),
    )
    for copy in copies:
        copy.start()
    copies[0].wait()
    base_cos = wave_ref[pl.ds(0, DEVICES), :]
    base_sin = wave_ref[pl.ds(DEVICES, DEVICES), :]
    for s in range(SLOTS):
        wave = (base_cos, base_sin)
        if s:
            turn_cos = wave_ref[pl.ds(2 * DEVICES + 2 * s, 1), :]
            turn_sin = wave_ref[pl.ds(2 * DEVICES + 2 * s + 1, 1), :]
            wave = (base_cos * turn_cos + base_sin * turn_sin, base_sin * turn_cos - base_cos * turn_sin)
        whi, wlo = split(jnp.concatenate(wave, axis=0))
        whi_ref[pl.ds(256 * s, 256), :] = whi
        wlo_ref[pl.ds(256 * s, 256), :] = wlo
    copies[1].wait()
    hi, lo = split(h_ref[0])
    order = band_order()
    hi_ref[...] = dot(order, hi).astype(bf16)
    lo_ref[...] = dot(order, lo).astype(bf16)


def forward_kernel(g_ref, own_hi_ref, own_lo_ref, whi_ref, wlo_ref, o_ref):
    lon_index = lax.axis_index("lon")
    order = band_order()
    got_hi, got_lo = split(g_ref[0])
    hi = jnp.concatenate([own_hi_ref[...], dot(order, got_hi).astype(bf16)], axis=0)
    lo = jnp.concatenate([own_lo_ref[...], dot(order, got_lo).astype(bf16)], axis=0)
    own_cos, own_sin = phases(lon_index)
    got_cos, got_sin = phases(lon_index ^ 1)
    lane = iota((DEVICES, LANES), 1)
    is_rest = lane // REST == MAIN // REST
    rest = jnp.zeros((DEVICES, LANES), f32)
    for s in range(SLOTS):
        whi = whi_ref[pl.ds(256 * s, 256), :]
        wlo = wlo_ref[pl.ds(256 * s, 256), :]
        terms = dot_nt(whi, hi) + (dot_nt(wlo, hi) + dot_nt(whi, lo))
        own_real, own_imag = turned_back(terms[:, :LANES], own_cos, own_sin)
        got_real, got_imag = turned_back(terms[:, LANES:], got_cos, got_sin)
        real, imag = own_real + got_real, own_imag + got_imag
        o_ref[pl.ds(s, DEVICES, stride=ROWS), :] = jnp.where(lane < MAIN, real, pltpu.roll(imag, MAIN, 1))
        for c, value in enumerate((real, imag)):
            shift = (REST * (s + 8 * c) - MAIN) % LANES
            kept = jnp.where(is_rest, value, 0.0)
            rest = rest + (pltpu.roll(kept, shift, 1) if shift else kept)
    o_ref[pl.ds(SLOTS, DEVICES, stride=ROWS), :] = rest


def legendre_kernel(
    coef_ref, tab_ref, phi_ref, plo_ref, phi_hbm, plo_hbm, phi_far, plo_far, stage_ref, sems
):
    device = lax.axis_index("lon") * LAT + lax.axis_index("lat")
    x = tab_ref[0]
    coarse = tab_ref[1]
    fine = tab_ref[2]
    lane = iota((1, DEVICES), 1)
    firsts, counts = [], []
    for s in range(SLOTS):
        order = (device + DEVICES * s).astype(f32)
        start = jnp.sum(jnp.where(lane == device, tab_ref[4, pl.ds(s, 1), :], 0.0), axis=1, keepdims=True)
        whole = order * coarse
        count = jnp.maximum(jnp.ceil(-whole * (1.0 / 60.0)), 0.0)
        firsts.append(jnp.exp2((whole + 60.0 * count) + (order * fine + start)))
        counts.append(count)
    zero = jnp.zeros((8, LANES), f32)
    state = [(zero, zero, counts[s]) for s in range(SLOTS)]
    copies = []
    for block in range(SLOTS):
        active = SLOTS - block

        def group(g, carried, block=block, active=active):
            carried = list(carried)
            factors = []
            for s in range(active):
                count = carried[3 * s + 2]
                factors.append(
                    jnp.where(
                        count < 0.5,
                        1.0,
                        jnp.where(count < 1.5, SMALL, jnp.where(count < 2.5, SMALL * SMALL, 0.0)),
                    )
                )
            for n in range(STEP):
                after = block * DEVICES + g * STEP + n
                for s in range(active):
                    earlier, latest = carried[3 * s], carried[3 * s + 1]
                    degree = DEVICES * s + after
                    growth = coef_ref[s * MODES + degree]
                    damped = coef_ref[(SLOTS + s) * MODES + degree]
                    current = (growth * x) * latest - damped * earlier
                    if block == 0:
                        current = jnp.where(after == device, firsts[s], current)
                    row = s * DEVICES * 8 + (g * STEP + n) * 8
                    stage_ref[pl.ds(pl.multiple_of(row, 8), 8), :] = current * factors[s]
                    carried[3 * s], carried[3 * s + 1] = latest, current
            for s in range(active):
                earlier, latest, count = carried[3 * s : 3 * s + 3]
                largest = jnp.maximum(jnp.abs(earlier), jnp.abs(latest))
                large = jnp.logical_and(largest > BIG, count > 0.5)
                scale = jnp.where(large, SMALL, 1.0)
                carried[3 * s] = earlier * scale
                carried[3 * s + 1] = latest * scale
                carried[3 * s + 2] = count - jnp.where(large, 1.0, 0.0)
            return tuple(carried)

        flat = tuple(v for s in range(active) for v in state[s])
        flat = lax.fori_loop(0, DEVICES // STEP, group, flat)
        for s in reversed(range(active)):
            state[s] = flat[3 * s : 3 * s + 3]
            first = SLOT_BASE[s] + block * DEVICES
            rows = pl.ds(first, DEVICES)
            hi_ref, lo_ref = (phi_ref, plo_ref) if s in KEPT else (phi_far, plo_far)
            for b in range(HALF + 1):
                piece = stage_ref[pl.ds(s * DEVICES * 8 + b, DEVICES, stride=8), :]
                hi, lo = split(piece)
                hi_ref[b, rows, :] = hi
                lo_ref[b, rows, :] = lo
            if s in SENT:
                for c, (near, far) in enumerate(((phi_far, phi_hbm), (plo_far, plo_hbm))):
                    copy = pltpu.make_async_copy(near.at[:, rows], far.at[:, rows], sems.at[c, block, SENT.index(s)])
                    copy.start()
                    copies.append(copy)
    for copy in copies:
        copy.wait()


def degree_kernel(
    t_ref,
    phi_ref,
    plo_ref,
    phi_hbm,
    plo_hbm,
    tab_ref,
    resp_ref,
    o_ref,
    phi_far,
    plo_far,
    sum_ref,
    fold_ref,
    rest_ref,
    back_ref,
    sems,
):
    copies = []
    for s in SENT:
        rows = pl.ds(SLOT_BASE[s], DEGREES[s])
        for c, (far, near) in enumerate(((phi_hbm, phi_far), (plo_hbm, plo_far))):
            copies.append(pltpu.make_async_copy(far.at[:, rows], near.at[:, rows], sems.at[c, SENT.index(s)]))
    for copy in copies:
        copy.start()
    device = lax.axis_index("lon") * LAT + lax.axis_index("lat")
    block = LAT * ROWS
    for c in range(2):
        total = t_ref[pl.ds(block * c, block), :]
        for i in range(1, PAIRS):
            total = total + t_ref[pl.ds(block * (2 * i + c), block), :]
        sum_ref[pl.ds(block * c, block), :] = total
    fold_ref[...] = jnp.zeros(fold_ref.shape, f32)
    own = iota((16, LANES), 1) // REST == iota((16, LANES), 0)
    first = iota((ROWS, LANES), 1) < MAIN
    for y in range(HALF):
        mains = []
        for c in range(2):
            upper = sum_ref[pl.ds(block * c + ROWS * y, ROWS), :]
            lower = sum_ref[pl.ds(block * c + ROWS * (LAT - 1 - y), ROWS), :]
            mains.append((upper + lower, upper - lower))
        lanes = slice(LANES * y, LANES * (y + 1))
        for p in range(2):
            left, right = mains[0][p], mains[1][p]
            weight = tab_ref[3, pl.ds(y, 1), :]
            fold_ref[pl.ds(16 * p, ROWS), lanes] = jnp.where(first, left, pltpu.roll(right, MAIN, 1)) * weight
            fold_ref[pl.ds(16 * p + 8, ROWS), lanes] = jnp.where(first, pltpu.roll(left, MAIN, 1), right) * weight
            for c in range(2):
                spread = jnp.where(own, mains[c][p][SLOTS : SLOTS + 1], 0.0)
                group = 2 * y + c
                rest_ref[pl.ds(16 * p, 16), LANES * group : LANES * (group + 1)] = spread
    lane_in = iota((LAT * LANES, LANES), 0)
    lane_out = iota((LAT * LANES, LANES), 1)
    place = ones_where(
        jnp.logical_and(lane_in % REST == lane_out % REST, lane_in // LANES == lane_out // REST)
    )
    rest_hi, rest_lo = split(rest_ref[...])
    rest = dot(rest_hi, place) + dot(rest_lo, place)
    fold_ref[:, DEPTH - LANES :] = rest * tab_ref[3, pl.ds(HALF, 1), :]
    fold_hi, fold_lo = split(fold_ref[...])
    both = jnp.concatenate([fold_hi, fold_lo], axis=0)
    back_ref[...] = jnp.zeros(back_ref.shape, f32)
    tables = [None] * SLOTS
    spectra = [None] * SLOTS
    for s in KEPT + SENT:
        if s == SENT[0]:
            for copy in copies:
                copy.wait()
        rows = pl.ds(SLOT_BASE[s], DEGREES[s])
        hi_ref, lo_ref = (phi_ref, plo_ref) if s in KEPT else (phi_far, plo_far)
        phi = jnp.concatenate([hi_ref[b, rows, :] for b in range(HALF + 1)], axis=1)
        plo = jnp.concatenate([lo_ref[b, rows, :] for b in range(HALF + 1)], axis=1)
        tables[s] = phi, plo
        main = dot_nt(both, phi)
        spectra[s] = main[:32] + (main[32:] + dot_nt(fold_hi, plo))
    for s in range(SLOTS):
        count = DEGREES[s]
        phi, plo = tables[s]
        terms = spectra[s]
        degree = iota((1, count), 1)
        even = ((degree + device) & 1) == 0
        weight = 2.0 if s else jnp.where(device == 0, 1.0, 2.0)
        factor = resp_ref[:, DEVICES * s :] * weight
        real = jnp.where(even, terms[s : s + 1], terms[16 + s : 17 + s]) * factor
        imag = jnp.where(even, terms[8 + s : 9 + s], terms[24 + s : 25 + s]) * factor
        four = jnp.concatenate(
            [
                jnp.where(even, real, 0.0),
                jnp.where(even, imag, 0.0),
                jnp.where(even, 0.0, real),
                jnp.where(even, 0.0, imag),
                jnp.zeros((4, count), f32),
            ],
            axis=0,
        )
        hi, lo = split(four)
        out = dot(jnp.concatenate([hi, lo], axis=0), phi)
        sums = out[:8] + (out[8:] + dot(hi, plo))
        for c in range(2):
            back_ref[pl.ds(8 * c + s, 1), :] = sums[c : c + 1] + sums[2 + c : 3 + c]
            back_ref[pl.ds(16 + 8 * c + s, 1), :] = sums[c : c + 1] - sums[2 + c : 3 + c]
    pick_in = iota((LANES, LAT * LANES), 0)
    pick_out = iota((LANES, LAT * LANES), 1)
    pick = ones_where(
        jnp.logical_and(pick_in % REST == pick_out % REST, pick_in // REST == pick_out // LANES)
    )
    rest_hi, rest_lo = split(back_ref[:, DEPTH - LANES :])
    rest = dot(rest_hi, pick) + dot(rest_lo, pick)
    for p in range(2):
        for y in range(HALF):
            band = y if p == 0 else LAT - 1 - y
            lanes = slice(LANES * y, LANES * (y + 1))
            real = back_ref[pl.ds(16 * p, ROWS), lanes]
            imag = back_ref[pl.ds(16 * p + 8, ROWS), lanes]
            for c in range(2):
                row = block * c + ROWS * band
                if c == 0:
                    sum_ref[pl.ds(row, ROWS), :] = jnp.where(first, real, pltpu.roll(imag, MAIN, 1))
                else:
                    sum_ref[pl.ds(row, ROWS), :] = jnp.where(first, pltpu.roll(real, MAIN, 1), imag)
                group = 2 * y + c
                kept = jnp.where(own, rest[16 * p : 16 * (p + 1), LANES * group : LANES * (group + 1)], 0.0)
                sum_ref[pl.ds(row + SLOTS, 1), :] = jnp.sum(kept, axis=0, keepdims=True)
    for c in range(2):
        total = sum_ref[pl.ds(block * c, block), :]
        for i in range(PAIRS):
            o_ref[pl.ds(block * (2 * i + c), block), :] = total


def half_inverse(ref, whi_ref, wlo_ref):
    cos, sin = phases(lax.axis_index("lon"))
    lane = iota((DEVICES, LANES), 1)
    is_main = lane < MAIN
    is_rest = lane // REST == MAIN // REST
    rest = ref[pl.ds(SLOTS, DEVICES, stride=ROWS), :]
    total = None
    for s in range(SLOTS):
        main = ref[pl.ds(s, DEVICES, stride=ROWS), :]
        parts = []
        for c in range(2):
            shift = (MAIN - REST * (s + 8 * c)) % LANES
            moved = pltpu.roll(rest, shift, 1) if shift else rest
            body = pltpu.roll(main, MAIN, 1) if c else main
            parts.append(jnp.where(is_main, body, jnp.where(is_rest, moved, 0.0)))
        real, imag = parts
        hi, lo = split(jnp.concatenate([real * cos - imag * sin, real * sin + imag * cos], axis=0))
        whi = whi_ref[:, 256 * s : 256 * (s + 1)]
        wlo = wlo_ref[:, 256 * s : 256 * (s + 1)]
        terms = dot(whi, hi) + (dot(wlo, hi) + dot(whi, lo))
        total = terms if total is None else total + terms
    return total


def own_inverse_kernel(r_ref, base_ref, turn_ref, o_ref, whi_ref, wlo_ref):
    base_cos = base_ref[:, :DEVICES]
    base_sin = base_ref[:, DEVICES:]
    for s in range(SLOTS):
        wave = (base_cos, base_sin)
        if s:
            turn_cos = turn_ref[pl.ds(2 * s * TURN, TURN), :]
            turn_sin = turn_ref[pl.ds((2 * s + 1) * TURN, TURN), :]
            turn_cos = jnp.concatenate([turn_cos] * (CELLS // TURN), axis=0)
            turn_sin = jnp.concatenate([turn_sin] * (CELLS // TURN), axis=0)
            wave = (base_cos * turn_cos + base_sin * turn_sin, base_sin * turn_cos - base_cos * turn_sin)
        whi, wlo = split(jnp.concatenate(wave, axis=1))
        whi_ref[:, 256 * s : 256 * (s + 1)] = whi
        wlo_ref[:, 256 * s : 256 * (s + 1)] = wlo
    o_ref[...] = half_inverse(r_ref, whi_ref, wlo_ref)


def inverse_kernel(g_ref, own_ref, whi_ref, wlo_ref, o_ref):
    part = lax.axis_index("lon") & 1
    north = lax.axis_index("lat") < HALF
    total = jnp.concatenate([own_ref[...], half_inverse(g_ref, whi_ref, wlo_ref)], axis=1)
    row = iota((BAND, 2 * LANES), 0)
    place = jnp.where(north, row, BAND - 1 - row) - PART * part
    mine = jnp.logical_and(place >= 0, place < PART)
    other = jnp.where(place < 0, place + PART, place - PART) + LANES
    order = ones_where(iota((BAND, 2 * LANES), 1) == jnp.where(mine, place, other))
    first, rest_of = split(total)
    second, third = split(total - first.astype(f32))
    o_ref[0] = dot_nt(order, first) + (dot_nt(order, second) + dot_nt(order, third))


def vmem(n):
    return [pl.BlockSpec(memory_space=pltpu.VMEM)] * n


def hbm(n):
    return [pl.BlockSpec(memory_space=pltpu.HBM)] * n


def limit(mib):
    return pltpu.CompilerParams(vmem_limit_bytes=mib * 2**20)


def in_hbm(x):
    return pltpu.with_memory_space_constraint(jnp.asarray(x), pltpu.HBM)


def swapped(x):
    return lax.ppermute(x, "lon", [(i, i ^ 1) for i in range(LON)])


def exchanged(x):
    x = x.reshape(DEVICES, 1, ROWS * LANES)
    x = lax.all_to_all(x, ("lon", "lat"), split_axis=0, concat_axis=0, tiled=True)
    return x.reshape(DEVICES * ROWS, LANES)


def recurrence_factors(device):
    degree = jnp.arange(MODES, dtype=jnp.int32)[None, :]
    order = (device + DEVICES * jnp.arange(SLOTS, dtype=jnp.int32))[:, None]
    started = degree > order
    l = degree.astype(f32)
    m = order.astype(f32)
    k = l - 1.0
    growth = jnp.where(started, jnp.sqrt((4.0 * l * l - 1.0) / jnp.where(started, l * l - m * m, 1.0)), 0.0)
    damping = jnp.sqrt(jnp.where(started, k * k - m * m, 0.0) / jnp.maximum(4.0 * k * k - 1.0, 1.0))
    return jnp.stack([growth, growth * damping]).reshape(2 * SLOTS * MODES)


def shards(height, response):
    device = lax.axis_index("lon") * LAT + lax.axis_index("lat")
    table = wave_table()
    tables = jnp.asarray(row_tables())
    packed = jax.ShapeDtypeStruct((DEVICES * ROWS, LANES), f32)
    got = swapped(height)
    kept = jax.ShapeDtypeStruct((HALF + 1, KEPT_ROWS, LANES), bf16)
    sent = pltpu.HBM((HALF + 1, SENT_ROWS, LANES), bf16)
    far = [pltpu.VMEM((HALF + 1, SENT_ROWS, LANES), bf16)] * 2
    near_hi, near_lo, far_hi, far_lo = pl.pallas_call(
        legendre_kernel,
        out_shape=(kept, kept, sent, sent),
        in_specs=[pl.BlockSpec(memory_space=pltpu.SMEM)] + vmem(1),
        out_specs=tuple(vmem(2) + hbm(2)),
        scratch_shapes=far
        + [
            pltpu.VMEM((SLOTS * DEVICES * 8, LANES), f32),
            pltpu.SemaphoreType.DMA((2, SLOTS, len(SENT))),
        ],
        compiler_params=limit(16),
        name="legendre",
    )(recurrence_factors(device), tables)
    operand = jax.ShapeDtypeStruct((LANES, CELLS), bf16)
    waves = jax.ShapeDtypeStruct((2 * MODES, CELLS), bf16)
    own_hi, own_lo, whi, wlo = pl.pallas_call(
        own_kernel,
        out_shape=(operand, operand, waves, waves),
        in_specs=hbm(2),
        out_specs=tuple(vmem(4)),
        scratch_shapes=[
            pltpu.VMEM((1, BAND, CELLS), f32),
            pltpu.VMEM((2 * DEVICES + 16, CELLS), f32),
            pltpu.SemaphoreType.DMA((2,)),
        ],
        compiler_params=limit(12),
        name="own_half",
    )(in_hbm(height), in_hbm(first_waves(table)))
    shares = pl.pallas_call(
        forward_kernel,
        out_shape=packed,
        in_specs=vmem(5),
        out_specs=vmem(1)[0],
        compiler_params=limit(12),
        name="forward_dft",
    )(got, own_hi, own_lo, whi, wlo)
    arrived = exchanged(shares)
    synthesis = pl.pallas_call(
        degree_kernel,
        out_shape=packed,
        in_specs=vmem(3) + hbm(2) + vmem(2),
        out_specs=vmem(1)[0],
        scratch_shapes=far
        + [
            pltpu.VMEM((2 * LAT * ROWS, LANES), f32),
            pltpu.VMEM((32, DEPTH), f32),
            pltpu.VMEM((32, LAT * LANES), f32),
            pltpu.VMEM((32, DEPTH), f32),
            pltpu.SemaphoreType.DMA((2, len(SENT))),
        ],
        compiler_params=limit(16),
        name="degrees",
    )(arrived, near_hi, near_lo, in_hbm(far_hi), in_hbm(far_lo), tables, response.reshape(1, MODES))
    returned = exchanged(synthesis)
    other = swapped(returned)
    waves = jax.ShapeDtypeStruct((CELLS, 2 * MODES), bf16)
    base, turns = last_waves(table)
    own, thi, tlo = pl.pallas_call(
        own_inverse_kernel,
        out_shape=(jax.ShapeDtypeStruct((CELLS, LANES), f32), waves, waves),
        in_specs=vmem(3),
        out_specs=tuple(vmem(3)),
        compiler_params=limit(12),
        name="own_inverse_dft",
    )(returned, jnp.asarray(base), jnp.asarray(turns))
    return pl.pallas_call(
        inverse_kernel,
        out_shape=jax.ShapeDtypeStruct((1, BAND, CELLS), f32),
        in_specs=vmem(4),
        out_specs=vmem(1)[0],
        compiler_params=limit(12),
        name="inverse_dft",
    )(other, own, thi, tlo)


def solution(mesh):
    placed = (P(None, "lat", "lon"), P())
    return jax.shard_map(
        shards, mesh=mesh, in_specs=placed, out_specs=P(None, "lat", "lon"), check_vma=False
    )
```

```python
import math

import numpy as np
import jax
import jax.numpy as jnp
from jax import lax
from jax.experimental import pallas as pl
from jax.experimental.pallas import tpu as pltpu
from jax.sharding import PartitionSpec as P

NLAT = 1152
NLON = 4096
MODES = 640
LON = 16
LAT = 8
DEVICES = LON * LAT
BAND = NLAT // LAT
CELLS = NLON // LON
SLOTS = MODES // DEVICES
LANES = 128
PART = BAND // 2
MAIN = 64
REST = PART - MAIN
ROWS = SLOTS + 1
PAIRS = LON // 2
HALF = LAT // 2
DEPTH = (HALF + 1) * LANES
STEP = 16
TURN = NLON // DEVICES
BIG = 2.0**60
SMALL = 2.0**-60

f32 = jnp.float32
bf16 = jnp.bfloat16

KEPT = (0, 1)
SENT = tuple(s for s in range(SLOTS) if s not in KEPT)
DEGREES = [MODES - DEVICES * s for s in range(SLOTS)]
SLOT_BASE = [sum(DEGREES[q] for q in (KEPT if s in KEPT else SENT) if q < s) for s in range(SLOTS)]
KEPT_ROWS = sum(DEGREES[s] for s in KEPT)
SENT_ROWS = sum(DEGREES[s] for s in SENT)


def split_np(x):
    x = np.asarray(x, np.float32)
    hi = x.astype(jnp.bfloat16)
    lo = (x - hi.astype(np.float32)).astype(jnp.bfloat16)
    return hi, lo


def wave_table():
    m = np.arange(MODES)[:, None]
    r = np.arange(CELLS)[None, :]
    angle = 2.0 * np.pi * ((m * r) % NLON) / NLON
    parts = np.stack([np.cos(angle), -np.sin(angle)]).reshape(2, SLOTS, DEVICES, CELLS)
    return parts.transpose(1, 0, 2, 3).reshape(2 * MODES, CELLS)


def first_waves(table):
    turns = 2.0 * np.pi * np.arange(8)[:, None] * np.arange(CELLS)[None, :] / TURN
    turns = np.stack([np.cos(turns), np.sin(turns)], axis=1).reshape(16, CELLS)
    return np.concatenate([table[: 2 * DEVICES], turns]).astype(np.float32)


def last_waves(table):
    turns = 2.0 * np.pi * np.arange(SLOTS)[:, None] * np.arange(TURN)[None, :] / TURN
    turns = np.stack([np.cos(turns), np.sin(turns)], axis=1).reshape(2 * SLOTS * TURN, 1)
    turns = np.broadcast_to(turns, (2 * SLOTS * TURN, LANES))
    return table[: 2 * DEVICES].T.astype(np.float32), turns.astype(np.float32)


def half_rows(values, fill):
    out = np.full((8, LANES), fill, np.float64)
    for y in range(HALF):
        for c in range(2):
            part = values[BAND * y + PART * c : BAND * y + PART * (c + 1)]
            out[y, MAIN * c : MAIN * (c + 1)] = part[:MAIN]
            first = REST * (2 * y + c)
            out[HALF, first : first + REST] = part[MAIN:]
    return out


def row_tables():
    theta = np.pi * (np.arange(NLAT // 2) + 0.5) / NLAT
    cosines = half_rows(np.cos(theta), 0.0)
    logs = half_rows(np.log2(np.sin(theta)), 0.0)
    weights = half_rows(np.sin(theta) * np.pi / NLAT * (2.0 * np.pi / NLON), 0.0)
    weights[HALF, MAIN:] = weights[HALF, :MAIN]
    coarse = np.round(logs * 4096.0) / 4096.0
    coarse = np.where(np.abs(logs) > 2.0, np.round(logs * 1024.0) / 1024.0, coarse)
    starts = [
        0.5 * (math.lgamma(m + 1.5) - math.lgamma(1.5) - math.lgamma(m + 1.0)) - 0.5 * math.log(4.0 * math.pi)
        for m in range(MODES)
    ]
    starts = np.zeros((8, DEVICES)) + np.pad(np.array(starts).reshape(SLOTS, DEVICES), ((0, 3), (0, 0))) / math.log(2.0)
    return np.stack([cosines, coarse, logs - coarse, weights, starts]).astype(np.float32)


def split(x):
    hi = x.astype(bf16)
    return hi, (x - hi.astype(f32)).astype(bf16)


def dot(a, b):
    return lax.dot_general(a, b, (((1,), (0,)), ((), ())), preferred_element_type=f32)


def dot_nt(a, b):
    return lax.dot_general(a, b, (((1,), (1,)), ((), ())), preferred_element_type=f32)


def iota(shape, dim):
    return lax.broadcasted_iota(jnp.int32, shape, dim)


def ones_where(cond):
    return jnp.where(cond, 1.0, 0.0).astype(bf16)


def phase_rows(lon_index):
    turn = (iota((16, LANES), 0) * lon_index) & 15
    angle = turn.astype(f32) * (2.0 * math.pi / 16)
    return jnp.cos(angle), jnp.sin(angle)


def tiled(rows):
    return jnp.concatenate([rows] * 8, axis=0)


def phases(lon_index):
    cos, sin = phase_rows(lon_index)
    return tiled(cos), tiled(sin)


def turned_back(terms, cos, sin):
    real, imag = terms[:DEVICES], terms[DEVICES:]
    return real * cos + imag * sin, imag * cos - real * sin


def band_order():
    part = lax.axis_index("lon") & 1
    north = lax.axis_index("lat") < HALF
    out_row = iota((LANES, BAND), 0)
    place = PART * part + out_row
    source = jnp.where(north, place, BAND - 1 - place)
    return ones_where(jnp.logical_and(iota((LANES, BAND), 1) == source, out_row < PART))


def own_kernel(
    h_hbm, wave_hbm, hi_ref, lo_ref, whi_ref, wlo_ref, phase_ref, order_ref, h_ref, wave_ref, sems
):
    copies = (
        pltpu.make_async_copy(wave_hbm, wave_ref, sems.at[0]),
        pltpu.make_async_copy(h_hbm, h_ref, sems.at[1]),
    )
    for copy in copies:
        copy.start()
    lon_index = lax.axis_index("lon")
    for n, rows in enumerate(phase_rows(lon_index) + phase_rows(lon_index ^ 1)):
        phase_ref[n] = rows
    order = band_order()
    order_ref[...] = order
    copies[0].wait()
    base_cos = wave_ref[pl.ds(0, DEVICES), :]
    base_sin = wave_ref[pl.ds(DEVICES, DEVICES), :]
    for s in range(SLOTS):
        wave = (base_cos, base_sin)
        if s:
            turn_cos = wave_ref[pl.ds(2 * DEVICES + 2 * s, 1), :]
            turn_sin = wave_ref[pl.ds(2 * DEVICES + 2 * s + 1, 1), :]
            wave = (base_cos * turn_cos + base_sin * turn_sin, base_sin * turn_cos - base_cos * turn_sin)
        whi, wlo = split(jnp.concatenate(wave, axis=0))
        whi_ref[pl.ds(256 * s, 256), :] = whi
        wlo_ref[pl.ds(256 * s, 256), :] = wlo
    copies[1].wait()
    hi, lo = split(h_ref[0])
    hi_ref[...] = dot(order, hi).astype(bf16)
    lo_ref[...] = dot(order, lo).astype(bf16)


def forward_kernel(g_ref, own_hi_ref, own_lo_ref, whi_ref, wlo_ref, phase_ref, order_ref, o_ref):
    order = order_ref[...]
    got_hi, got_lo = split(g_ref[0])
    hi = jnp.concatenate([own_hi_ref[...], dot(order, got_hi).astype(bf16)], axis=0)
    lo = jnp.concatenate([own_lo_ref[...], dot(order, got_lo).astype(bf16)], axis=0)
    own_cos, own_sin, got_cos, got_sin = (tiled(phase_ref[n]) for n in range(4))
    lane = iota((DEVICES, LANES), 1)
    is_rest = lane // REST == MAIN // REST
    rest = jnp.zeros((DEVICES, LANES), f32)
    waves = jnp.concatenate([whi_ref[...], wlo_ref[...], whi_ref[...]], axis=1)
    all_terms = dot_nt(waves, jnp.concatenate([hi, hi, lo], axis=1))
    for s in range(SLOTS):
        terms = all_terms[256 * s : 256 * (s + 1)]
        own_real, own_imag = turned_back(terms[:, :LANES], own_cos, own_sin)
        got_real, got_imag = turned_back(terms[:, LANES:], got_cos, got_sin)
        real, imag = own_real + got_real, own_imag + got_imag
        o_ref[pl.ds(s, DEVICES, stride=ROWS), :] = jnp.where(lane < MAIN, real, pltpu.roll(imag, MAIN, 1))
        for c, value in enumerate((real, imag)):
            shift = (REST * (s + 8 * c) - MAIN) % LANES
            kept = jnp.where(is_rest, value, 0.0)
            rest = rest + (pltpu.roll(kept, shift, 1) if shift else kept)
    o_ref[pl.ds(SLOTS, DEVICES, stride=ROWS), :] = rest


def legendre_kernel(coef_ref, tab_ref, near_ref, far_hbm, far_ref, stage_ref, sems):
    device = lax.axis_index("lon") * LAT + lax.axis_index("lat")
    x = tab_ref[0]
    coarse = tab_ref[1]
    fine = tab_ref[2]
    lane = iota((1, DEVICES), 1)
    used = jnp.logical_or(iota((8, LANES), 0) < HALF, iota((8, LANES), 1) < MAIN)
    firsts, counts = [], []
    for s in range(SLOTS):
        order = (device + DEVICES * s).astype(f32)
        start = jnp.sum(jnp.where(lane == device, tab_ref[4, pl.ds(s, 1), :], 0.0), axis=1, keepdims=True)
        whole = order * coarse
        count = jnp.maximum(jnp.ceil(-whole * (1.0 / 60.0)), 0.0)
        firsts.append(jnp.where(used, jnp.exp2((whole + 60.0 * count) + (order * fine + start)), 0.0))
        counts.append(count)
    zero = jnp.zeros((8, LANES), f32)
    state = [(zero, zero, counts[s]) for s in range(SLOTS)]
    copies = []
    for block in range(SLOTS):
        active = SLOTS - block

        def group(g, carried, block=block, active=active):
            carried = list(carried)
            factors = []
            for s in range(active):
                count = carried[3 * s + 2]
                factors.append(
                    jnp.where(
                        count < 0.5,
                        1.0,
                        jnp.where(count < 1.5, SMALL, jnp.where(count < 2.5, SMALL * SMALL, 0.0)),
                    )
                )
            for n in range(STEP):
                after = block * DEVICES + g * STEP + n
                for s in range(active):
                    earlier, latest = carried[3 * s], carried[3 * s + 1]
                    degree = DEVICES * s + after
                    growth = coef_ref[s * MODES + degree]
                    damped = coef_ref[(SLOTS + s) * MODES + degree]
                    current = (growth * x) * latest - damped * earlier
                    if block == 0:
                        current = jnp.where(after == device, firsts[s], current)
                    row = s * DEVICES * 8 + (g * STEP + n) * 8
                    stage_ref[pl.ds(pl.multiple_of(row, 8), 8), :] = current * factors[s]
                    carried[3 * s], carried[3 * s + 1] = latest, current
            for s in range(active):
                earlier, latest, count = carried[3 * s : 3 * s + 3]
                largest = jnp.maximum(jnp.abs(earlier), jnp.abs(latest))
                large = jnp.logical_and(largest > BIG, count > 0.5)
                scale = jnp.where(large, SMALL, 1.0)
                carried[3 * s] = earlier * scale
                carried[3 * s + 1] = latest * scale
                carried[3 * s + 2] = count - jnp.where(large, 1.0, 0.0)
            return tuple(carried)

        flat = tuple(v for s in range(active) for v in state[s])
        flat = lax.fori_loop(0, DEVICES // STEP, group, flat)
        for s in reversed(range(active)):
            state[s] = flat[3 * s : 3 * s + 3]
            first = SLOT_BASE[s] + block * DEVICES
            rows = pl.ds(first, DEVICES)
            ref = near_ref if s in KEPT else far_ref
            for b in range(HALF + 1):
                hi, lo = split(stage_ref[pl.ds(s * DEVICES * 8 + b, DEVICES, stride=8), :])
                if b < HALF:
                    ref[b, rows, :] = hi
                    ref[HALF + b, rows, :] = lo
                else:
                    ref[2 * HALF, rows, :] = (hi.astype(f32) + pltpu.roll(lo.astype(f32), MAIN, 1)).astype(bf16)
            if s in SENT:
                copy = pltpu.make_async_copy(
                    far_ref.at[:, rows], far_hbm.at[:, rows], sems.at[block, SENT.index(s)]
                )
                copy.start()
                copies.append(copy)
    for copy in copies:
        copy.wait()


def degree_kernel(
    t_ref,
    near_ref,
    far_hbm,
    tab_ref,
    resp_ref,
    o_ref,
    far_ref,
    sum_ref,
    fold_ref,
    rest_ref,
    back_ref,
    sems,
):
    copies = []
    for s in SENT:
        rows = pl.ds(SLOT_BASE[s], DEGREES[s])
        copies.append(
            pltpu.make_async_copy(far_hbm.at[:, rows], far_ref.at[:, rows], sems.at[SENT.index(s)])
        )
    for copy in copies:
        copy.start()
    device = lax.axis_index("lon") * LAT + lax.axis_index("lat")
    block = LAT * ROWS
    for c in range(2):
        total = t_ref[pl.ds(block * c, block), :]
        for i in range(1, PAIRS):
            total = total + t_ref[pl.ds(block * (2 * i + c), block), :]
        sum_ref[pl.ds(block * c, block), :] = total
    fold_ref[...] = jnp.zeros(fold_ref.shape, f32)
    own = iota((16, LANES), 1) // REST == iota((16, LANES), 0)
    first = iota((ROWS, LANES), 1) < MAIN
    for y in range(HALF):
        mains = []
        for c in range(2):
            upper = sum_ref[pl.ds(block * c + ROWS * y, ROWS), :]
            lower = sum_ref[pl.ds(block * c + ROWS * (LAT - 1 - y), ROWS), :]
            mains.append((upper + lower, upper - lower))
        lanes = slice(LANES * y, LANES * (y + 1))
        for p in range(2):
            left, right = mains[0][p], mains[1][p]
            weight = tab_ref[3, pl.ds(y, 1), :]
            fold_ref[pl.ds(16 * p, ROWS), lanes] = jnp.where(first, left, pltpu.roll(right, MAIN, 1)) * weight
            fold_ref[pl.ds(16 * p + 8, ROWS), lanes] = jnp.where(first, pltpu.roll(left, MAIN, 1), right) * weight
            for c in range(2):
                spread = jnp.where(own, mains[c][p][SLOTS : SLOTS + 1], 0.0)
                group = 2 * y + c
                rest_ref[pl.ds(16 * p, 16), LANES * group : LANES * (group + 1)] = spread
    spreader = ones_where(iota((LANES, LANES), 0) % REST == iota((LANES, LANES), 1) % REST)
    lane_in = iota((LAT * LANES, LANES), 0)
    lane_out = iota((LAT * LANES, LANES), 1)
    place = ones_where(
        jnp.logical_and(lane_in % REST == lane_out % REST, lane_in // LANES == lane_out // REST % LAT)
    )
    rest_hi, rest_lo = split(rest_ref[...])
    rest = dot(rest_hi, place) + dot(rest_lo, place)
    fold_ref[:, DEPTH - LANES :] = rest * tab_ref[3, pl.ds(HALF, 1), :]
    fold_hi, fold_lo = split(fold_ref[...])
    below = iota((32, DEPTH), 1) < DEPTH - MAIN
    both = jnp.concatenate([fold_hi, jnp.where(below, fold_lo, jnp.zeros_like(fold_lo))], axis=0)
    main_hi = fold_hi[:, : DEPTH - LANES]
    back_ref[...] = jnp.zeros(back_ref.shape, f32)
    tables = [None] * SLOTS
    spectra = [None] * SLOTS
    for s in KEPT + SENT:
        if s == SENT[0]:
            for copy in copies:
                copy.wait()
        rows = pl.ds(SLOT_BASE[s], DEGREES[s])
        ref = near_ref if s in KEPT else far_ref
        phi = jnp.concatenate([ref[b, rows, :] for b in (*range(HALF), 2 * HALF)], axis=1)
        plo = jnp.concatenate([ref[HALF + b, rows, :] for b in range(HALF)], axis=1)
        tables[s] = phi, plo
        main = dot_nt(both, phi)
        spectra[s] = main[:32] + (main[32:] + dot_nt(main_hi, plo))
    for s in range(SLOTS):
        count = DEGREES[s]
        phi, plo = tables[s]
        terms = spectra[s]
        degree = iota((1, count), 1)
        even = ((degree + device) & 1) == 0
        weight = 2.0 if s else jnp.where(device == 0, 1.0, 2.0)
        factor = resp_ref[:, DEVICES * s :] * weight
        real = jnp.where(even, terms[s : s + 1], terms[16 + s : 17 + s]) * factor
        imag = jnp.where(even, terms[8 + s : 9 + s], terms[24 + s : 25 + s]) * factor
        four = jnp.concatenate(
            [
                jnp.where(even, real, 0.0),
                jnp.where(even, imag, 0.0),
                jnp.where(even, 0.0, real),
                jnp.where(even, 0.0, imag),
                jnp.zeros((4, count), f32),
            ],
            axis=0,
        )
        hi, lo = split(four)
        out = dot(jnp.concatenate([hi, lo], axis=0), phi)
        both_rest = out[:8, DEPTH - LANES :]
        lower = jnp.concatenate([dot(hi, plo), pltpu.roll(both_rest, MAIN, 1)], axis=1)
        sums = out[:8] + (out[8:] + lower)
        for c in range(2):
            back_ref[pl.ds(8 * c + s, 1), :] = sums[c : c + 1] + sums[2 + c : 3 + c]
            back_ref[pl.ds(16 + 8 * c + s, 1), :] = sums[c : c + 1] - sums[2 + c : 3 + c]
    packed = back_ref[:, DEPTH - LANES :]
    group = iota((32, LANES), 1) // REST
    rest_hi, rest_lo = split(
        jnp.concatenate([jnp.where(group == g, packed, 0.0) for g in range(LAT)], axis=0)
    )
    rest = dot(rest_hi, spreader) + dot(rest_lo, spreader)
    for p in range(2):
        for y in range(HALF):
            band = y if p == 0 else LAT - 1 - y
            lanes = slice(LANES * y, LANES * (y + 1))
            real = back_ref[pl.ds(16 * p, ROWS), lanes]
            imag = back_ref[pl.ds(16 * p + 8, ROWS), lanes]
            for c in range(2):
                row = block * c + ROWS * band
                if c == 0:
                    sum_ref[pl.ds(row, ROWS), :] = jnp.where(first, real, pltpu.roll(imag, MAIN, 1))
                else:
                    sum_ref[pl.ds(row, ROWS), :] = jnp.where(first, pltpu.roll(real, MAIN, 1), imag)
                row_of = 32 * (2 * y + c) + 16 * p
                kept = jnp.where(own, rest[row_of : row_of + 16], 0.0)
                sum_ref[pl.ds(row + SLOTS, 1), :] = jnp.sum(kept, axis=0, keepdims=True)
    for c in range(2):
        total = sum_ref[pl.ds(block * c, block), :]
        for i in range(PAIRS):
            o_ref[pl.ds(block * (2 * i + c), block), :] = total


def half_inverse(ref, cos, sin, whi_ref, wlo_ref):
    lane = iota((DEVICES, LANES), 1)
    is_main = lane < MAIN
    is_rest = lane // REST == MAIN // REST
    rest = ref[pl.ds(SLOTS, DEVICES, stride=ROWS), :]
    total = None
    for s in range(SLOTS):
        main = ref[pl.ds(s, DEVICES, stride=ROWS), :]
        parts = []
        for c in range(2):
            shift = (MAIN - REST * (s + 8 * c)) % LANES
            moved = pltpu.roll(rest, shift, 1) if shift else rest
            body = pltpu.roll(main, MAIN, 1) if c else main
            parts.append(jnp.where(is_main, body, jnp.where(is_rest, moved, 0.0)))
        real, imag = parts
        pair = jnp.concatenate(split(jnp.concatenate([real * cos - imag * sin, real * sin + imag * cos], axis=0)), axis=1)
        whi = whi_ref[:, 256 * s : 256 * (s + 1)]
        wlo = wlo_ref[:, 256 * s : 256 * (s + 1)]
        terms = dot(whi, pair) + dot(wlo, pair)
        total = terms if total is None else total + terms
    return total[:, :LANES] + total[:, LANES:]


def placed(heights, owner):
    part = (lax.axis_index("lon") & 1) ^ owner
    north = lax.axis_index("lat") < HALF
    row = iota((BAND, LANES), 0)
    place = jnp.where(north, row, BAND - 1 - row) - PART * part
    inside = jnp.logical_and(place >= 0, place < PART)
    order = ones_where(jnp.logical_and(iota((BAND, LANES), 1) == place, inside))
    first = heights.astype(bf16)
    second, third = split(heights - first.astype(f32))
    return dot_nt(order, first) + (dot_nt(order, second) + dot_nt(order, third))


def own_inverse_kernel(r_ref, base_ref, turn_ref, o_ref, phase_ref, whi_ref, wlo_ref):
    base_cos = base_ref[:, :DEVICES]
    base_sin = base_ref[:, DEVICES:]
    for s in range(SLOTS):
        wave = (base_cos, base_sin)
        if s:
            turn_cos = turn_ref[pl.ds(2 * s * TURN, TURN), :]
            turn_sin = turn_ref[pl.ds((2 * s + 1) * TURN, TURN), :]
            turn_cos = jnp.concatenate([turn_cos] * (CELLS // TURN), axis=0)
            turn_sin = jnp.concatenate([turn_sin] * (CELLS // TURN), axis=0)
            wave = (base_cos * turn_cos + base_sin * turn_sin, base_sin * turn_cos - base_cos * turn_sin)
        whi, wlo = split(jnp.concatenate(wave, axis=1))
        whi_ref[:, 256 * s : 256 * (s + 1)] = whi
        wlo_ref[:, 256 * s : 256 * (s + 1)] = wlo
    cos, sin = phases(lax.axis_index("lon"))
    phase_ref[0] = cos
    phase_ref[1] = sin
    o_ref[...] = placed(half_inverse(r_ref, cos, sin, whi_ref, wlo_ref), 0)


def inverse_kernel(g_ref, own_ref, phase_ref, whi_ref, wlo_ref, o_ref):
    heights = half_inverse(g_ref, phase_ref[0], phase_ref[1], whi_ref, wlo_ref)
    o_ref[0] = own_ref[...] + placed(heights, 1)


def vmem(n):
    return [pl.BlockSpec(memory_space=pltpu.VMEM)] * n


def hbm(n):
    return [pl.BlockSpec(memory_space=pltpu.HBM)] * n


def limit(mib):
    return pltpu.CompilerParams(vmem_limit_bytes=mib * 2**20)


def in_hbm(x):
    return pltpu.with_memory_space_constraint(jnp.asarray(x), pltpu.HBM)


def swapped(x):
    return lax.ppermute(x, "lon", [(i, i ^ 1) for i in range(LON)])


def exchanged(x):
    x = x.reshape(DEVICES, 1, ROWS * LANES)
    x = lax.all_to_all(x, ("lon", "lat"), split_axis=0, concat_axis=0, tiled=True)
    return x.reshape(DEVICES * ROWS, LANES)


def recurrence_factors(device):
    degree = jnp.arange(MODES, dtype=jnp.int32)[None, :]
    order = (device + DEVICES * jnp.arange(SLOTS, dtype=jnp.int32))[:, None]
    started = degree > order
    l = degree.astype(f32)
    m = order.astype(f32)
    k = l - 1.0
    growth = jnp.where(started, jnp.sqrt((4.0 * l * l - 1.0) / jnp.where(started, l * l - m * m, 1.0)), 0.0)
    damping = jnp.sqrt(jnp.where(started, k * k - m * m, 0.0) / jnp.maximum(4.0 * k * k - 1.0, 1.0))
    return jnp.stack([growth, growth * damping]).reshape(2 * SLOTS * MODES)


def shards(height, response):
    device = lax.axis_index("lon") * LAT + lax.axis_index("lat")
    table = wave_table()
    tables = jnp.asarray(row_tables())
    packed = jax.ShapeDtypeStruct((DEVICES * ROWS, LANES), f32)
    got = swapped(height)
    kept = jax.ShapeDtypeStruct((2 * HALF + 1, KEPT_ROWS, LANES), bf16)
    sent = pltpu.HBM((2 * HALF + 1, SENT_ROWS, LANES), bf16)
    far = [pltpu.VMEM((2 * HALF + 1, SENT_ROWS, LANES), bf16)]
    near_legendre, far_legendre = pl.pallas_call(
        legendre_kernel,
        out_shape=(kept, sent),
        in_specs=[pl.BlockSpec(memory_space=pltpu.SMEM)] + vmem(1),
        out_specs=tuple(vmem(1) + hbm(1)),
        scratch_shapes=far
        + [
            pltpu.VMEM((SLOTS * DEVICES * 8, LANES), f32),
            pltpu.SemaphoreType.DMA((SLOTS, len(SENT))),
        ],
        compiler_params=limit(16),
        name="legendre",
    )(recurrence_factors(device), tables)
    operand = jax.ShapeDtypeStruct((LANES, CELLS), bf16)
    waves = jax.ShapeDtypeStruct((2 * MODES, CELLS), bf16)
    own_half = pl.pallas_call(
        own_kernel,
        out_shape=(
            operand,
            operand,
            waves,
            waves,
            jax.ShapeDtypeStruct((4, 16, LANES), f32),
            jax.ShapeDtypeStruct((LANES, BAND), bf16),
        ),
        in_specs=hbm(2),
        out_specs=tuple(vmem(6)),
        scratch_shapes=[
            pltpu.VMEM((1, BAND, CELLS), f32),
            pltpu.VMEM((2 * DEVICES + 16, CELLS), f32),
            pltpu.SemaphoreType.DMA((2,)),
        ],
        compiler_params=limit(12),
        name="own_half",
    )(in_hbm(height), in_hbm(first_waves(table)))
    shares = pl.pallas_call(
        forward_kernel,
        out_shape=packed,
        in_specs=vmem(7),
        out_specs=vmem(1)[0],
        compiler_params=limit(12),
        name="forward_dft",
    )(got, *own_half)
    arrived = exchanged(shares)
    synthesis = pl.pallas_call(
        degree_kernel,
        out_shape=packed,
        in_specs=vmem(2) + hbm(1) + vmem(2),
        out_specs=vmem(1)[0],
        scratch_shapes=far
        + [
            pltpu.VMEM((2 * LAT * ROWS, LANES), f32),
            pltpu.VMEM((32, DEPTH), f32),
            pltpu.VMEM((32, LAT * LANES), f32),
            pltpu.VMEM((32, DEPTH), f32),
            pltpu.SemaphoreType.DMA((len(SENT),)),
        ],
        compiler_params=limit(16),
        name="degrees",
    )(arrived, near_legendre, in_hbm(far_legendre), tables, response.reshape(1, MODES))
    returned = exchanged(synthesis)
    other = swapped(returned)
    waves = jax.ShapeDtypeStruct((CELLS, 2 * MODES), bf16)
    base, turns = last_waves(table)
    own, phase, thi, tlo = pl.pallas_call(
        own_inverse_kernel,
        out_shape=(
            jax.ShapeDtypeStruct((BAND, CELLS), f32),
            jax.ShapeDtypeStruct((2, DEVICES, LANES), f32),
            waves,
            waves,
        ),
        in_specs=vmem(3),
        out_specs=tuple(vmem(4)),
        compiler_params=limit(12),
        name="own_inverse_dft",
    )(returned, jnp.asarray(base), jnp.asarray(turns))
    return pl.pallas_call(
        inverse_kernel,
        out_shape=jax.ShapeDtypeStruct((1, BAND, CELLS), f32),
        in_specs=vmem(5),
        out_specs=vmem(1)[0],
        compiler_params=limit(12),
        name="inverse_dft",
    )(other, own, phase, thi, tlo)


def solution(mesh):
    placed = (P(None, "lat", "lon"), P())
    return jax.shard_map(
        shards, mesh=mesh, in_specs=placed, out_specs=P(None, "lat", "lon"), check_vma=False
    )
```

```python
import math

import numpy as np
import jax
import jax.numpy as jnp
from jax import lax
from jax.experimental import pallas as pl
from jax.experimental.pallas import tpu as pltpu
from jax.sharding import PartitionSpec as P

NLAT = 1152
NLON = 4096
MODES = 640
LON = 16
LAT = 8
DEVICES = LON * LAT
BAND = NLAT // LAT
CELLS = NLON // LON
SLOTS = MODES // DEVICES
LANES = 128
PART = BAND // 2
MAIN = 64
REST = PART - MAIN
ROWS = SLOTS + 1
PAIRS = LON // 2
HALF = LAT // 2
DEPTH = (HALF + 1) * LANES
STEP = 16
TURN = NLON // DEVICES
BIG = 2.0**60
SMALL = 2.0**-60

f32 = jnp.float32
bf16 = jnp.bfloat16

KEPT = (0, 1)
SENT = tuple(s for s in range(SLOTS) if s not in KEPT)
DEGREES = [MODES - DEVICES * s for s in range(SLOTS)]
SLOT_BASE = [sum(DEGREES[q] for q in (KEPT if s in KEPT else SENT) if q < s) for s in range(SLOTS)]
KEPT_ROWS = sum(DEGREES[s] for s in KEPT)
SENT_ROWS = sum(DEGREES[s] for s in SENT)


def split_np(x):
    x = np.asarray(x, np.float32)
    hi = x.astype(jnp.bfloat16)
    lo = (x - hi.astype(np.float32)).astype(jnp.bfloat16)
    return hi, lo


def wave_table():
    m = np.arange(MODES)[:, None]
    r = np.arange(CELLS)[None, :]
    angle = 2.0 * np.pi * ((m * r) % NLON) / NLON
    parts = np.stack([np.cos(angle), -np.sin(angle)]).reshape(2, SLOTS, DEVICES, CELLS)
    return parts.transpose(1, 0, 2, 3).reshape(2 * MODES, CELLS)


def first_waves(table):
    turns = 2.0 * np.pi * np.arange(8)[:, None] * np.arange(CELLS)[None, :] / TURN
    turns = np.stack([np.cos(turns), np.sin(turns)], axis=1).reshape(16, CELLS)
    return np.concatenate([table[: 2 * DEVICES], turns]).astype(np.float32)


def last_waves(table):
    turns = 2.0 * np.pi * np.arange(SLOTS)[:, None] * np.arange(TURN)[None, :] / TURN
    turns = np.stack([np.cos(turns), np.sin(turns)], axis=1).reshape(2 * SLOTS * TURN, 1)
    turns = np.broadcast_to(turns, (2 * SLOTS * TURN, LANES))
    return table[: 2 * DEVICES].T.astype(np.float32), turns.astype(np.float32)


def half_rows(values, fill):
    out = np.full((8, LANES), fill, np.float64)
    for y in range(HALF):
        for c in range(2):
            part = values[BAND * y + PART * c : BAND * y + PART * (c + 1)]
            out[y, MAIN * c : MAIN * (c + 1)] = part[:MAIN]
            first = REST * (2 * y + c)
            out[HALF, first : first + REST] = part[MAIN:]
    return out


def row_tables():
    theta = np.pi * (np.arange(NLAT // 2) + 0.5) / NLAT
    cosines = half_rows(np.cos(theta), 0.0)
    logs = half_rows(np.log2(np.sin(theta)), 0.0)
    weights = half_rows(np.sin(theta) * np.pi / NLAT * (2.0 * np.pi / NLON), 0.0)
    weights[HALF, MAIN:] = weights[HALF, :MAIN]
    coarse = np.round(logs * 4096.0) / 4096.0
    coarse = np.where(np.abs(logs) > 2.0, np.round(logs * 1024.0) / 1024.0, coarse)
    starts = [
        0.5 * (math.lgamma(m + 1.5) - math.lgamma(1.5) - math.lgamma(m + 1.0)) - 0.5 * math.log(4.0 * math.pi)
        for m in range(MODES)
    ]
    starts = np.zeros((8, DEVICES)) + np.pad(np.array(starts).reshape(SLOTS, DEVICES), ((0, 3), (0, 0))) / math.log(2.0)
    return np.stack([cosines, coarse, logs - coarse, weights, starts]).astype(np.float32)


def split(x):
    hi = x.astype(bf16)
    return hi, (x - hi.astype(f32)).astype(bf16)


def dot(a, b):
    return lax.dot_general(a, b, (((1,), (0,)), ((), ())), preferred_element_type=f32)


def dot_nt(a, b):
    return lax.dot_general(a, b, (((1,), (1,)), ((), ())), preferred_element_type=f32)


def iota(shape, dim):
    return lax.broadcasted_iota(jnp.int32, shape, dim)


def ones_where(cond):
    return jnp.where(cond, 1.0, 0.0).astype(bf16)


def phase_rows(lon_index):
    turn = (iota((16, LANES), 0) * lon_index) & 15
    angle = turn.astype(f32) * (2.0 * math.pi / 16)
    return jnp.cos(angle), jnp.sin(angle)


def tiled(rows):
    return jnp.concatenate([rows] * 8, axis=0)


def phases(lon_index):
    cos, sin = phase_rows(lon_index)
    return tiled(cos), tiled(sin)


def turned_back(terms, cos, sin):
    real, imag = terms[:DEVICES], terms[DEVICES:]
    return real * cos + imag * sin, imag * cos - real * sin


def band_order():
    part = lax.axis_index("lon") & 1
    north = lax.axis_index("lat") < HALF
    out_row = iota((LANES, BAND), 0)
    place = PART * part + out_row
    source = jnp.where(north, place, BAND - 1 - place)
    return ones_where(jnp.logical_and(iota((LANES, BAND), 1) == source, out_row < PART))


def own_kernel(
    h_hbm, wave_hbm, hi_ref, lo_ref, whi_ref, wlo_ref, phase_ref, order_ref, h_ref, wave_ref, sems
):
    copies = (
        pltpu.make_async_copy(wave_hbm, wave_ref, sems.at[0]),
        pltpu.make_async_copy(h_hbm, h_ref, sems.at[1]),
    )
    for copy in copies:
        copy.start()
    lon_index = lax.axis_index("lon")
    for n, rows in enumerate(phase_rows(lon_index) + phase_rows(lon_index ^ 1)):
        phase_ref[n] = rows
    order = band_order()
    order_ref[...] = order
    copies[0].wait()
    base_cos = wave_ref[pl.ds(0, DEVICES), :]
    base_sin = wave_ref[pl.ds(DEVICES, DEVICES), :]
    for s in range(SLOTS):
        wave = (base_cos, base_sin)
        if s:
            turn_cos = wave_ref[pl.ds(2 * DEVICES + 2 * s, 1), :]
            turn_sin = wave_ref[pl.ds(2 * DEVICES + 2 * s + 1, 1), :]
            wave = (base_cos * turn_cos + base_sin * turn_sin, base_sin * turn_cos - base_cos * turn_sin)
        whi, wlo = split(jnp.concatenate(wave, axis=0))
        whi_ref[pl.ds(256 * s, 256), :] = whi
        wlo_ref[pl.ds(256 * s, 256), :] = wlo
    copies[1].wait()
    hi, lo = split(h_ref[0])
    hi_ref[...] = dot(order, hi).astype(bf16)
    lo_ref[...] = dot(order, lo).astype(bf16)


def forward_kernel(g_ref, own_hi_ref, own_lo_ref, whi_ref, wlo_ref, phase_ref, order_ref, o_ref):
    order = order_ref[...]
    got_hi, got_lo = split(g_ref[0])
    hi = jnp.concatenate([own_hi_ref[...], dot(order, got_hi).astype(bf16)], axis=0)
    lo = jnp.concatenate([own_lo_ref[...], dot(order, got_lo).astype(bf16)], axis=0)
    own_cos, own_sin, got_cos, got_sin = (tiled(phase_ref[n]) for n in range(4))
    lane = iota((DEVICES, LANES), 1)
    is_rest = lane // REST == MAIN // REST
    rest = jnp.zeros((DEVICES, LANES), f32)
    waves = jnp.concatenate([whi_ref[...], wlo_ref[...], whi_ref[...]], axis=1)
    all_terms = dot_nt(waves, jnp.concatenate([hi, hi, lo], axis=1))
    for s in range(SLOTS):
        terms = all_terms[256 * s : 256 * (s + 1)]
        own_real, own_imag = turned_back(terms[:, :LANES], own_cos, own_sin)
        got_real, got_imag = turned_back(terms[:, LANES:], got_cos, got_sin)
        real, imag = own_real + got_real, own_imag + got_imag
        o_ref[pl.ds(s, DEVICES, stride=ROWS), :] = jnp.where(lane < MAIN, real, pltpu.roll(imag, MAIN, 1))
        for c, value in enumerate((real, imag)):
            shift = (REST * (s + 8 * c) - MAIN) % LANES
            kept = jnp.where(is_rest, value, 0.0)
            rest = rest + (pltpu.roll(kept, shift, 1) if shift else kept)
    o_ref[pl.ds(SLOTS, DEVICES, stride=ROWS), :] = rest


def legendre_kernel(coef_ref, tab_ref, near_ref, far_hbm, far_ref, stage_ref, sems):
    device = lax.axis_index("lon") * LAT + lax.axis_index("lat")
    x = tab_ref[0]
    coarse = tab_ref[1]
    fine = tab_ref[2]
    lane = iota((1, DEVICES), 1)
    used = jnp.logical_or(iota((8, LANES), 0) < HALF, iota((8, LANES), 1) < MAIN)
    firsts, counts = [], []
    for s in range(SLOTS):
        order = (device + DEVICES * s).astype(f32)
        start = jnp.sum(jnp.where(lane == device, tab_ref[4, pl.ds(s, 1), :], 0.0), axis=1, keepdims=True)
        whole = order * coarse
        count = jnp.maximum(jnp.ceil(-whole * (1.0 / 60.0)), 0.0)
        firsts.append(jnp.where(used, jnp.exp2((whole + 60.0 * count) + (order * fine + start)), 0.0))
        counts.append(count)
    zero = jnp.zeros((8, LANES), f32)
    state = [(zero, zero, counts[s]) for s in range(SLOTS)]
    copies = []
    for block in range(SLOTS):
        active = SLOTS - block

        def group(g, carried, block=block, active=active):
            carried = list(carried)
            factors = []
            for s in range(active):
                count = carried[3 * s + 2]
                factors.append(
                    jnp.where(
                        count < 0.5,
                        1.0,
                        jnp.where(count < 1.5, SMALL, jnp.where(count < 2.5, SMALL * SMALL, 0.0)),
                    )
                )
            for n in range(STEP):
                after = block * DEVICES + g * STEP + n
                for s in range(active):
                    earlier, latest = carried[3 * s], carried[3 * s + 1]
                    degree = DEVICES * s + after
                    growth = coef_ref[s * MODES + degree]
                    damped = coef_ref[(SLOTS + s) * MODES + degree]
                    current = (growth * x) * latest - damped * earlier
                    if block == 0:
                        current = jnp.where(after == device, firsts[s], current)
                    row = s * DEVICES * 8 + (g * STEP + n) * 8
                    stage_ref[pl.ds(pl.multiple_of(row, 8), 8), :] = current * factors[s]
                    carried[3 * s], carried[3 * s + 1] = latest, current
            for s in range(active):
                earlier, latest, count = carried[3 * s : 3 * s + 3]
                largest = jnp.maximum(jnp.abs(earlier), jnp.abs(latest))
                large = jnp.logical_and(largest > BIG, count > 0.5)
                scale = jnp.where(large, SMALL, 1.0)
                carried[3 * s] = earlier * scale
                carried[3 * s + 1] = latest * scale
                carried[3 * s + 2] = count - jnp.where(large, 1.0, 0.0)
            return tuple(carried)

        flat = tuple(v for s in range(active) for v in state[s])
        flat = lax.fori_loop(0, DEVICES // STEP, group, flat)
        for s in reversed(range(active)):
            state[s] = flat[3 * s : 3 * s + 3]
            first = SLOT_BASE[s] + block * DEVICES
            rows = pl.ds(first, DEVICES)
            ref = near_ref if s in KEPT else far_ref
            for b in range(HALF + 1):
                hi, lo = split(stage_ref[pl.ds(s * DEVICES * 8 + b, DEVICES, stride=8), :])
                if b < HALF:
                    ref[b, rows, :] = hi
                    ref[HALF + b, rows, :] = lo
                else:
                    ref[2 * HALF, rows, :] = (hi.astype(f32) + pltpu.roll(lo.astype(f32), MAIN, 1)).astype(bf16)
            if s in SENT:
                copy = pltpu.make_async_copy(
                    far_ref.at[:, rows], far_hbm.at[:, rows], sems.at[block, SENT.index(s)]
                )
                copy.start()
                copies.append(copy)
    for copy in copies:
        copy.wait()


def degree_kernel(
    t_ref,
    near_ref,
    far_hbm,
    tab_ref,
    resp_ref,
    o_ref,
    far_ref,
    sum_ref,
    fold_ref,
    rest_ref,
    back_ref,
    sems,
):
    copies = []
    for s in SENT:
        rows = pl.ds(SLOT_BASE[s], DEGREES[s])
        copies.append(
            pltpu.make_async_copy(far_hbm.at[:, rows], far_ref.at[:, rows], sems.at[SENT.index(s)])
        )
    for copy in copies:
        copy.start()
    device = lax.axis_index("lon") * LAT + lax.axis_index("lat")
    block = LAT * ROWS
    for c in range(2):
        total = t_ref[pl.ds(block * c, block), :]
        for i in range(1, PAIRS):
            total = total + t_ref[pl.ds(block * (2 * i + c), block), :]
        sum_ref[pl.ds(block * c, block), :] = total
    fold_ref[...] = jnp.zeros(fold_ref.shape, f32)
    own = iota((16, LANES), 1) // REST == iota((16, LANES), 0)
    first = iota((ROWS, LANES), 1) < MAIN
    for y in range(HALF):
        mains = []
        for c in range(2):
            upper = sum_ref[pl.ds(block * c + ROWS * y, ROWS), :]
            lower = sum_ref[pl.ds(block * c + ROWS * (LAT - 1 - y), ROWS), :]
            mains.append((upper + lower, upper - lower))
        lanes = slice(LANES * y, LANES * (y + 1))
        for p in range(2):
            left, right = mains[0][p], mains[1][p]
            weight = tab_ref[3, pl.ds(y, 1), :]
            fold_ref[pl.ds(16 * p, ROWS), lanes] = jnp.where(first, left, pltpu.roll(right, MAIN, 1)) * weight
            fold_ref[pl.ds(16 * p + 8, ROWS), lanes] = jnp.where(first, pltpu.roll(left, MAIN, 1), right) * weight
            for c in range(2):
                spread = jnp.where(own, mains[c][p][SLOTS : SLOTS + 1], 0.0)
                group = 2 * y + c
                rest_ref[pl.ds(16 * p, 16), LANES * group : LANES * (group + 1)] = spread
    spreader = ones_where(iota((LANES, LANES), 0) % REST == iota((LANES, LANES), 1) % REST)
    lane_in = iota((LAT * LANES, LANES), 0)
    lane_out = iota((LAT * LANES, LANES), 1)
    place = ones_where(
        jnp.logical_and(lane_in % REST == lane_out % REST, lane_in // LANES == lane_out // REST % LAT)
    )
    rest_hi, rest_lo = split(rest_ref[...])
    rest = dot(rest_hi, place) + dot(rest_lo, place)
    fold_ref[:, DEPTH - LANES :] = rest * tab_ref[3, pl.ds(HALF, 1), :]
    fold_hi, fold_lo = split(fold_ref[...])
    below = iota((32, DEPTH), 1) < DEPTH - MAIN
    both = jnp.concatenate([fold_hi, jnp.where(below, fold_lo, jnp.zeros_like(fold_lo))], axis=0)
    main_hi = fold_hi[:, : DEPTH - LANES]
    back_ref[...] = jnp.zeros(back_ref.shape, f32)
    tables = [None] * SLOTS
    spectra = [None] * SLOTS
    for s in KEPT + SENT:
        if s == SENT[0]:
            for copy in copies:
                copy.wait()
        rows = pl.ds(SLOT_BASE[s], DEGREES[s])
        ref = near_ref if s in KEPT else far_ref
        phi = jnp.concatenate([ref[b, rows, :] for b in (*range(HALF), 2 * HALF)], axis=1)
        plo = jnp.concatenate([ref[HALF + b, rows, :] for b in range(HALF)], axis=1)
        tables[s] = phi, plo
        main = dot_nt(both, phi)
        spectra[s] = main[:32] + (main[32:] + dot_nt(main_hi, plo))
    for s in range(SLOTS):
        count = DEGREES[s]
        phi, plo = tables[s]
        terms = spectra[s]
        degree = iota((1, count), 1)
        even = ((degree + device) & 1) == 0
        weight = 2.0 if s else jnp.where(device == 0, 1.0, 2.0)
        factor = resp_ref[:, DEVICES * s :] * weight
        real = jnp.where(even, terms[s : s + 1], terms[16 + s : 17 + s]) * factor
        imag = jnp.where(even, terms[8 + s : 9 + s], terms[24 + s : 25 + s]) * factor
        four = jnp.concatenate(
            [
                jnp.where(even, real, 0.0),
                jnp.where(even, imag, 0.0),
                jnp.where(even, 0.0, real),
                jnp.where(even, 0.0, imag),
                jnp.zeros((4, count), f32),
            ],
            axis=0,
        )
        hi, lo = split(four)
        out = dot(jnp.concatenate([hi, lo], axis=0), phi)
        both_rest = out[:8, DEPTH - LANES :]
        lower = jnp.concatenate([dot(hi, plo), pltpu.roll(both_rest, MAIN, 1)], axis=1)
        sums = out[:8] + (out[8:] + lower)
        for c in range(2):
            back_ref[pl.ds(8 * c + s, 1), :] = sums[c : c + 1] + sums[2 + c : 3 + c]
            back_ref[pl.ds(16 + 8 * c + s, 1), :] = sums[c : c + 1] - sums[2 + c : 3 + c]
    packed = back_ref[:, DEPTH - LANES :]
    group = iota((32, LANES), 1) // REST
    rest_hi, rest_lo = split(
        jnp.concatenate([jnp.where(group == g, packed, 0.0) for g in range(LAT)], axis=0)
    )
    rest = dot(rest_hi, spreader) + dot(rest_lo, spreader)
    for p in range(2):
        for y in range(HALF):
            band = y if p == 0 else LAT - 1 - y
            lanes = slice(LANES * y, LANES * (y + 1))
            real = back_ref[pl.ds(16 * p, ROWS), lanes]
            imag = back_ref[pl.ds(16 * p + 8, ROWS), lanes]
            for c in range(2):
                row = block * c + ROWS * band
                if c == 0:
                    sum_ref[pl.ds(row, ROWS), :] = jnp.where(first, real, pltpu.roll(imag, MAIN, 1))
                else:
                    sum_ref[pl.ds(row, ROWS), :] = jnp.where(first, pltpu.roll(real, MAIN, 1), imag)
                row_of = 32 * (2 * y + c) + 16 * p
                kept = jnp.where(own, rest[row_of : row_of + 16], 0.0)
                sum_ref[pl.ds(row + SLOTS, 1), :] = jnp.sum(kept, axis=0, keepdims=True)
    for c in range(2):
        total = sum_ref[pl.ds(block * c, block), :]
        for i in range(PAIRS):
            o_ref[pl.ds(block * (2 * i + c), block), :] = total


def half_inverse(ref, cos, sin, whi_ref, wlo_ref):
    lane = iota((DEVICES, LANES), 1)
    is_main = lane < MAIN
    is_rest = lane // REST == MAIN // REST
    rest = ref[pl.ds(SLOTS, DEVICES, stride=ROWS), :]
    total = None
    for s in range(SLOTS):
        main = ref[pl.ds(s, DEVICES, stride=ROWS), :]
        parts = []
        for c in range(2):
            shift = (MAIN - REST * (s + 8 * c)) % LANES
            moved = pltpu.roll(rest, shift, 1) if shift else rest
            body = pltpu.roll(main, MAIN, 1) if c else main
            parts.append(jnp.where(is_main, body, jnp.where(is_rest, moved, 0.0)))
        real, imag = parts
        pair = jnp.concatenate(split(jnp.concatenate([real * cos - imag * sin, real * sin + imag * cos], axis=0)), axis=1)
        whi = whi_ref[:, 256 * s : 256 * (s + 1)]
        wlo = wlo_ref[:, 256 * s : 256 * (s + 1)]
        terms = dot(whi, pair) + dot(wlo, pair)
        total = terms if total is None else total + terms
    return total[:, :LANES] + total[:, LANES:]


def placed(heights, owner):
    part = (lax.axis_index("lon") & 1) ^ owner
    north = lax.axis_index("lat") < HALF
    row = iota((BAND, LANES), 0)
    place = jnp.where(north, row, BAND - 1 - row) - PART * part
    inside = jnp.logical_and(place >= 0, place < PART)
    order = ones_where(jnp.logical_and(iota((BAND, LANES), 1) == place, inside))
    first = heights.astype(bf16)
    second, third = split(heights - first.astype(f32))
    return dot_nt(order, first) + (dot_nt(order, second) + dot_nt(order, third))


def own_inverse_kernel(r_ref, base_ref, turn_ref, o_ref, phase_ref, whi_ref, wlo_ref):
    base_cos = base_ref[:, :DEVICES]
    base_sin = base_ref[:, DEVICES:]
    for s in range(SLOTS):
        wave = (base_cos, base_sin)
        if s:
            turn_cos = turn_ref[pl.ds(2 * s * TURN, TURN), :]
            turn_sin = turn_ref[pl.ds((2 * s + 1) * TURN, TURN), :]
            turn_cos = jnp.concatenate([turn_cos] * (CELLS // TURN), axis=0)
            turn_sin = jnp.concatenate([turn_sin] * (CELLS // TURN), axis=0)
            wave = (base_cos * turn_cos + base_sin * turn_sin, base_sin * turn_cos - base_cos * turn_sin)
        whi, wlo = split(jnp.concatenate(wave, axis=1))
        whi_ref[:, 256 * s : 256 * (s + 1)] = whi
        wlo_ref[:, 256 * s : 256 * (s + 1)] = wlo
    cos, sin = phases(lax.axis_index("lon"))
    phase_ref[0] = cos
    phase_ref[1] = sin
    o_ref[...] = placed(half_inverse(r_ref, cos, sin, whi_ref, wlo_ref), 0)


def inverse_kernel(g_ref, own_ref, phase_ref, whi_ref, wlo_ref, o_ref):
    heights = half_inverse(g_ref, phase_ref[0], phase_ref[1], whi_ref, wlo_ref)
    o_ref[0] = own_ref[...] + placed(heights, 1)


def vmem(n):
    return [pl.BlockSpec(memory_space=pltpu.VMEM)] * n


def hbm(n):
    return [pl.BlockSpec(memory_space=pltpu.HBM)] * n


def limit(mib):
    return pltpu.CompilerParams(vmem_limit_bytes=mib * 2**20)


def in_hbm(x):
    return pltpu.with_memory_space_constraint(jnp.asarray(x), pltpu.HBM)


def swapped(x):
    return lax.ppermute(x, "lon", [(i, i ^ 1) for i in range(LON)])


def exchanged(x):
    x = x.reshape(DEVICES, 1, ROWS * LANES)
    x = lax.all_to_all(x, ("lon", "lat"), split_axis=0, concat_axis=0, tiled=True)
    return x.reshape(DEVICES * ROWS, LANES)


def recurrence_factors(device):
    degree = jnp.arange(MODES, dtype=jnp.int32)[None, :]
    order = (device + DEVICES * jnp.arange(SLOTS, dtype=jnp.int32))[:, None]
    started = degree > order
    l = degree.astype(f32)
    m = order.astype(f32)
    k = l - 1.0
    growth = jnp.where(started, jnp.sqrt((4.0 * l * l - 1.0) / jnp.where(started, l * l - m * m, 1.0)), 0.0)
    damping = jnp.sqrt(jnp.where(started, k * k - m * m, 0.0) / jnp.maximum(4.0 * k * k - 1.0, 1.0))
    return jnp.stack([growth, growth * damping]).reshape(2 * SLOTS * MODES)


def shards(height, response):
    device = lax.axis_index("lon") * LAT + lax.axis_index("lat")
    table = wave_table()
    tables = jnp.asarray(row_tables())
    packed = jax.ShapeDtypeStruct((DEVICES * ROWS, LANES), f32)
    got = swapped(height)
    kept = jax.ShapeDtypeStruct((2 * HALF + 1, KEPT_ROWS, LANES), bf16)
    sent = pltpu.HBM((2 * HALF + 1, SENT_ROWS, LANES), bf16)
    far = [pltpu.VMEM((2 * HALF + 1, SENT_ROWS, LANES), bf16)]
    near_legendre, far_legendre = pl.pallas_call(
        legendre_kernel,
        out_shape=(kept, sent),
        in_specs=[pl.BlockSpec(memory_space=pltpu.SMEM)] + vmem(1),
        out_specs=tuple(vmem(1) + hbm(1)),
        scratch_shapes=far
        + [
            pltpu.VMEM((SLOTS * DEVICES * 8, LANES), f32),
            pltpu.SemaphoreType.DMA((SLOTS, len(SENT))),
        ],
        compiler_params=limit(16),
        name="legendre",
    )(recurrence_factors(device), tables)
    operand = jax.ShapeDtypeStruct((LANES, CELLS), bf16)
    waves = jax.ShapeDtypeStruct((2 * MODES, CELLS), bf16)
    own_half = pl.pallas_call(
        own_kernel,
        out_shape=(
            operand,
            operand,
            waves,
            waves,
            jax.ShapeDtypeStruct((4, 16, LANES), f32),
            jax.ShapeDtypeStruct((LANES, BAND), bf16),
        ),
        in_specs=hbm(2),
        out_specs=tuple(vmem(6)),
        scratch_shapes=[
            pltpu.VMEM((1, BAND, CELLS), f32),
            pltpu.VMEM((2 * DEVICES + 16, CELLS), f32),
            pltpu.SemaphoreType.DMA((2,)),
        ],
        compiler_params=limit(12),
        name="own_half",
    )(in_hbm(height), in_hbm(first_waves(table)))
    shares = pl.pallas_call(
        forward_kernel,
        out_shape=packed,
        in_specs=vmem(7),
        out_specs=vmem(1)[0],
        compiler_params=limit(12),
        name="forward_dft",
    )(got, *own_half)
    arrived = exchanged(shares)
    synthesis = pl.pallas_call(
        degree_kernel,
        out_shape=packed,
        in_specs=vmem(2) + hbm(1) + vmem(2),
        out_specs=vmem(1)[0],
        scratch_shapes=far
        + [
            pltpu.VMEM((2 * LAT * ROWS, LANES), f32),
            pltpu.VMEM((32, DEPTH), f32),
            pltpu.VMEM((32, LAT * LANES), f32),
            pltpu.VMEM((32, DEPTH), f32),
            pltpu.SemaphoreType.DMA((len(SENT),)),
        ],
        compiler_params=pltpu.CompilerParams(
            vmem_limit_bytes=16 * 2**20,
        ),
        name="degrees",
    )(arrived, near_legendre, in_hbm(far_legendre), tables, response.reshape(1, MODES))
    returned = exchanged(synthesis)
    other = swapped(returned)
    waves = jax.ShapeDtypeStruct((CELLS, 2 * MODES), bf16)
    base, turns = last_waves(table)
    own, phase, thi, tlo = pl.pallas_call(
        own_inverse_kernel,
        out_shape=(
            jax.ShapeDtypeStruct((BAND, CELLS), f32),
            jax.ShapeDtypeStruct((2, DEVICES, LANES), f32),
            waves,
            waves,
        ),
        in_specs=vmem(3),
        out_specs=tuple(vmem(4)),
        compiler_params=limit(12),
        name="own_inverse_dft",
    )(returned, jnp.asarray(base), jnp.asarray(turns))
    return pl.pallas_call(
        inverse_kernel,
        out_shape=jax.ShapeDtypeStruct((1, BAND, CELLS), f32),
        in_specs=vmem(5),
        out_specs=vmem(1)[0],
        compiler_params=limit(12),
        name="inverse_dft",
    )(other, own, phase, thi, tlo)


def solution(mesh):
    placed = (P(None, "lat", "lon"), P())
    return jax.shard_map(
        shards, mesh=mesh, in_specs=placed, out_specs=P(None, "lat", "lon"), check_vma=False
    )
```

```python
import math

import numpy as np
import jax
import jax.numpy as jnp
from jax import lax
from jax.experimental import pallas as pl
from jax.experimental.pallas import tpu as pltpu
from jax.sharding import PartitionSpec as P

NLAT = 1152
NLON = 4096
MODES = 640
LON = 16
LAT = 8
DEVICES = LON * LAT
BAND = NLAT // LAT
CELLS = NLON // LON
SLOTS = MODES // DEVICES
LANES = 128
PART = BAND // 2
MAIN = 64
REST = PART - MAIN
ROWS = SLOTS + 1
PAIRS = LON // 2
HALF = LAT // 2
DEPTH = (HALF + 1) * LANES
STEP = 16
TURN = NLON // DEVICES
BIG = 2.0**60
SMALL = 2.0**-60

f32 = jnp.float32
bf16 = jnp.bfloat16

KEPT = (0, 1)
SENT = tuple(s for s in range(SLOTS) if s not in KEPT)
DEGREES = [MODES - DEVICES * s for s in range(SLOTS)]
SLOT_BASE = [sum(DEGREES[q] for q in (KEPT if s in KEPT else SENT) if q < s) for s in range(SLOTS)]
KEPT_ROWS = sum(DEGREES[s] for s in KEPT)
SENT_ROWS = sum(DEGREES[s] for s in SENT)


def split_np(x):
    x = np.asarray(x, np.float32)
    hi = x.astype(jnp.bfloat16)
    lo = (x - hi.astype(np.float32)).astype(jnp.bfloat16)
    return hi, lo


def wave_table():
    m = np.arange(MODES)[:, None]
    r = np.arange(CELLS)[None, :]
    angle = 2.0 * np.pi * ((m * r) % NLON) / NLON
    parts = np.stack([np.cos(angle), -np.sin(angle)]).reshape(2, SLOTS, DEVICES, CELLS)
    return parts.transpose(1, 0, 2, 3).reshape(2 * MODES, CELLS)


def first_waves(table):
    turns = 2.0 * np.pi * np.arange(8)[:, None] * np.arange(CELLS)[None, :] / TURN
    turns = np.stack([np.cos(turns), np.sin(turns)], axis=1).reshape(16, CELLS)
    return np.concatenate([table[: 2 * DEVICES], turns]).astype(np.float32)


def last_waves(table):
    turns = 2.0 * np.pi * np.arange(SLOTS)[:, None] * np.arange(TURN)[None, :] / TURN
    turns = np.stack([np.cos(turns), np.sin(turns)], axis=1).reshape(2 * SLOTS * TURN, 1)
    turns = np.broadcast_to(turns, (2 * SLOTS * TURN, LANES))
    return table[: 2 * DEVICES].T.astype(np.float32), turns.astype(np.float32)


def half_rows(values, fill):
    out = np.full((8, LANES), fill, np.float64)
    for y in range(HALF):
        for c in range(2):
            part = values[BAND * y + PART * c : BAND * y + PART * (c + 1)]
            out[y, MAIN * c : MAIN * (c + 1)] = part[:MAIN]
            first = REST * (2 * y + c)
            out[HALF, first : first + REST] = part[MAIN:]
    return out


def row_tables():
    theta = np.pi * (np.arange(NLAT // 2) + 0.5) / NLAT
    cosines = half_rows(np.cos(theta), 0.0)
    logs = half_rows(np.log2(np.sin(theta)), 0.0)
    weights = half_rows(np.sin(theta) * np.pi / NLAT * (2.0 * np.pi / NLON), 0.0)
    weights[HALF, MAIN:] = weights[HALF, :MAIN]
    coarse = np.round(logs * 4096.0) / 4096.0
    coarse = np.where(np.abs(logs) > 2.0, np.round(logs * 1024.0) / 1024.0, coarse)
    starts = [
        0.5 * (math.lgamma(m + 1.5) - math.lgamma(1.5) - math.lgamma(m + 1.0)) - 0.5 * math.log(4.0 * math.pi)
        for m in range(MODES)
    ]
    starts = np.zeros((8, DEVICES)) + np.pad(np.array(starts).reshape(SLOTS, DEVICES), ((0, 3), (0, 0))) / math.log(2.0)
    return np.stack([cosines, coarse, logs - coarse, weights, starts]).astype(np.float32)


def split(x):
    hi = x.astype(bf16)
    return hi, (x - hi.astype(f32)).astype(bf16)


def dot(a, b):
    return lax.dot_general(a, b, (((1,), (0,)), ((), ())), preferred_element_type=f32)


def dot_nt(a, b):
    return lax.dot_general(a, b, (((1,), (1,)), ((), ())), preferred_element_type=f32)


def iota(shape, dim):
    return lax.broadcasted_iota(jnp.int32, shape, dim)


def ones_where(cond):
    return jnp.where(cond, 1.0, 0.0).astype(bf16)


def phase_rows(lon_index):
    turn = (iota((16, LANES), 0) * lon_index) & 15
    angle = turn.astype(f32) * (2.0 * math.pi / 16)
    return jnp.cos(angle), jnp.sin(angle)


def tiled(rows):
    return jnp.concatenate([rows] * 8, axis=0)


def phases(lon_index):
    cos, sin = phase_rows(lon_index)
    return tiled(cos), tiled(sin)


def turned_back(terms, cos, sin):
    real, imag = terms[:DEVICES], terms[DEVICES:]
    return real * cos + imag * sin, imag * cos - real * sin


def band_order():
    part = lax.axis_index("lon") & 1
    north = lax.axis_index("lat") < HALF
    out_row = iota((LANES, BAND), 0)
    place = PART * part + out_row
    source = jnp.where(north, place, BAND - 1 - place)
    return ones_where(jnp.logical_and(iota((LANES, BAND), 1) == source, out_row < PART))


def own_kernel(
    h_hbm, wave_hbm, hi_ref, lo_ref, whi_ref, wlo_ref, phase_ref, order_ref, h_ref, wave_ref, sems
):
    copies = (
        pltpu.make_async_copy(wave_hbm, wave_ref, sems.at[0]),
        pltpu.make_async_copy(h_hbm, h_ref, sems.at[1]),
    )
    for copy in copies:
        copy.start()
    lon_index = lax.axis_index("lon")
    for n, rows in enumerate(phase_rows(lon_index) + phase_rows(lon_index ^ 1)):
        phase_ref[n] = rows
    order = band_order()
    order_ref[...] = order
    copies[0].wait()
    base_cos = wave_ref[pl.ds(0, DEVICES), :]
    base_sin = wave_ref[pl.ds(DEVICES, DEVICES), :]
    for s in range(SLOTS):
        wave = (base_cos, base_sin)
        if s:
            turn_cos = wave_ref[pl.ds(2 * DEVICES + 2 * s, 1), :]
            turn_sin = wave_ref[pl.ds(2 * DEVICES + 2 * s + 1, 1), :]
            wave = (base_cos * turn_cos + base_sin * turn_sin, base_sin * turn_cos - base_cos * turn_sin)
        whi, wlo = split(jnp.concatenate(wave, axis=0))
        whi_ref[pl.ds(256 * s, 256), :] = whi
        wlo_ref[pl.ds(256 * s, 256), :] = wlo
    copies[1].wait()
    hi, lo = split(h_ref[0])
    hi_ref[...] = dot(order, hi).astype(bf16)
    lo_ref[...] = dot(order, lo).astype(bf16)


def forward_kernel(g_ref, own_hi_ref, own_lo_ref, whi_ref, wlo_ref, phase_ref, order_ref, o_ref):
    order = order_ref[...]
    got_hi, got_lo = split(g_ref[0])
    hi = jnp.concatenate([own_hi_ref[...], dot(order, got_hi).astype(bf16)], axis=0)
    lo = jnp.concatenate([own_lo_ref[...], dot(order, got_lo).astype(bf16)], axis=0)
    own_cos, own_sin, got_cos, got_sin = (tiled(phase_ref[n]) for n in range(4))
    lane = iota((DEVICES, LANES), 1)
    is_rest = lane // REST == MAIN // REST
    rest = jnp.zeros((DEVICES, LANES), f32)
    waves = jnp.concatenate([whi_ref[...], wlo_ref[...], whi_ref[...]], axis=1)
    all_terms = dot_nt(waves, jnp.concatenate([hi, hi, lo], axis=1))
    for s in range(SLOTS):
        terms = all_terms[256 * s : 256 * (s + 1)]
        own_real, own_imag = turned_back(terms[:, :LANES], own_cos, own_sin)
        got_real, got_imag = turned_back(terms[:, LANES:], got_cos, got_sin)
        real, imag = own_real + got_real, own_imag + got_imag
        o_ref[pl.ds(s, DEVICES, stride=ROWS), :] = jnp.where(lane < MAIN, real, pltpu.roll(imag, MAIN, 1))
        for c, value in enumerate((real, imag)):
            shift = (REST * (s + 8 * c) - MAIN) % LANES
            kept = jnp.where(is_rest, value, 0.0)
            rest = rest + (pltpu.roll(kept, shift, 1) if shift else kept)
    o_ref[pl.ds(SLOTS, DEVICES, stride=ROWS), :] = rest


def legendre_kernel(coef_ref, tab_ref, near_ref, far_hbm, far_ref, stage_ref, sems):
    device = lax.axis_index("lon") * LAT + lax.axis_index("lat")
    x = tab_ref[0]
    coarse = tab_ref[1]
    fine = tab_ref[2]
    lane = iota((1, DEVICES), 1)
    used = jnp.logical_or(iota((8, LANES), 0) < HALF, iota((8, LANES), 1) < MAIN)
    firsts, counts = [], []
    for s in range(SLOTS):
        order = (device + DEVICES * s).astype(f32)
        start = jnp.sum(jnp.where(lane == device, tab_ref[4, pl.ds(s, 1), :], 0.0), axis=1, keepdims=True)
        whole = order * coarse
        count = jnp.maximum(jnp.ceil(-whole * (1.0 / 60.0)), 0.0)
        firsts.append(jnp.where(used, jnp.exp2((whole + 60.0 * count) + (order * fine + start)), 0.0))
        counts.append(count)
    zero = jnp.zeros((8, LANES), f32)
    state = [(zero, zero, counts[s]) for s in range(SLOTS)]
    copies = []
    for block in range(SLOTS):
        active = SLOTS - block

        def group(g, carried, block=block, active=active):
            carried = list(carried)
            factors = []
            for s in range(active):
                count = carried[3 * s + 2]
                factors.append(
                    jnp.where(
                        count < 0.5,
                        1.0,
                        jnp.where(count < 1.5, SMALL, jnp.where(count < 2.5, SMALL * SMALL, 0.0)),
                    )
                )
            for n in range(STEP):
                after = block * DEVICES + g * STEP + n
                for s in range(active):
                    earlier, latest = carried[3 * s], carried[3 * s + 1]
                    degree = DEVICES * s + after
                    growth = coef_ref[s * MODES + degree]
                    damped = coef_ref[(SLOTS + s) * MODES + degree]
                    current = (growth * x) * latest - damped * earlier
                    if block == 0:
                        current = jnp.where(after == device, firsts[s], current)
                    row = s * DEVICES * 8 + (g * STEP + n) * 8
                    stage_ref[pl.ds(pl.multiple_of(row, 8), 8), :] = current * factors[s]
                    carried[3 * s], carried[3 * s + 1] = latest, current
            for s in range(active):
                earlier, latest, count = carried[3 * s : 3 * s + 3]
                largest = jnp.maximum(jnp.abs(earlier), jnp.abs(latest))
                large = jnp.logical_and(largest > BIG, count > 0.5)
                scale = jnp.where(large, SMALL, 1.0)
                carried[3 * s] = earlier * scale
                carried[3 * s + 1] = latest * scale
                carried[3 * s + 2] = count - jnp.where(large, 1.0, 0.0)
            return tuple(carried)

        flat = tuple(v for s in range(active) for v in state[s])
        flat = lax.fori_loop(0, DEVICES // STEP, group, flat)
        for s in reversed(range(active)):
            state[s] = flat[3 * s : 3 * s + 3]
            first = SLOT_BASE[s] + block * DEVICES
            rows = pl.ds(first, DEVICES)
            ref = near_ref if s in KEPT else far_ref
            for b in range(HALF + 1):
                hi, lo = split(stage_ref[pl.ds(s * DEVICES * 8 + b, DEVICES, stride=8), :])
                if b < HALF:
                    ref[b, rows, :] = hi
                    ref[HALF + b, rows, :] = lo
                else:
                    ref[2 * HALF, rows, :] = (hi.astype(f32) + pltpu.roll(lo.astype(f32), MAIN, 1)).astype(bf16)
            if s in SENT:
                copy = pltpu.make_async_copy(
                    far_ref.at[:, rows], far_hbm.at[:, rows], sems.at[block, SENT.index(s)]
                )
                copy.start()
                copies.append(copy)
    for copy in copies:
        copy.wait()


def degree_kernel(
    t_ref,
    near_ref,
    far_hbm,
    tab_ref,
    resp_ref,
    o_ref,
    far_ref,
    sum_ref,
    fold_ref,
    rest_ref,
    back_ref,
    sems,
):
    copies = []
    for s in SENT:
        rows = pl.ds(SLOT_BASE[s], DEGREES[s])
        copies.append(
            pltpu.make_async_copy(far_hbm.at[:, rows], far_ref.at[:, rows], sems.at[SENT.index(s)])
        )
    for copy in copies:
        copy.start()
    device = lax.axis_index("lon") * LAT + lax.axis_index("lat")
    block = LAT * ROWS
    for c in range(2):
        total = t_ref[pl.ds(block * c, block), :]
        for i in range(1, PAIRS):
            total = total + t_ref[pl.ds(block * (2 * i + c), block), :]
        sum_ref[pl.ds(block * c, block), :] = total
    fold_ref[...] = jnp.zeros(fold_ref.shape, f32)
    own = iota((16, LANES), 1) // REST == iota((16, LANES), 0)
    first = iota((ROWS, LANES), 1) < MAIN
    for y in range(HALF):
        mains = []
        for c in range(2):
            upper = sum_ref[pl.ds(block * c + ROWS * y, ROWS), :]
            lower = sum_ref[pl.ds(block * c + ROWS * (LAT - 1 - y), ROWS), :]
            mains.append((upper + lower, upper - lower))
        lanes = slice(LANES * y, LANES * (y + 1))
        for p in range(2):
            left, right = mains[0][p], mains[1][p]
            weight = tab_ref[3, pl.ds(y, 1), :]
            fold_ref[pl.ds(16 * p, ROWS), lanes] = jnp.where(first, left, pltpu.roll(right, MAIN, 1)) * weight
            fold_ref[pl.ds(16 * p + 8, ROWS), lanes] = jnp.where(first, pltpu.roll(left, MAIN, 1), right) * weight
            for c in range(2):
                spread = jnp.where(own, mains[c][p][SLOTS : SLOTS + 1], 0.0)
                group = 2 * y + c
                rest_ref[pl.ds(16 * p, 16), LANES * group : LANES * (group + 1)] = spread
    spreader = ones_where(iota((LANES, LANES), 0) % REST == iota((LANES, LANES), 1) % REST)
    lane_in = iota((LAT * LANES, LANES), 0)
    lane_out = iota((LAT * LANES, LANES), 1)
    place = ones_where(
        jnp.logical_and(lane_in % REST == lane_out % REST, lane_in // LANES == lane_out // REST % LAT)
    )
    rest_hi, rest_lo = split(rest_ref[...])
    rest = dot(rest_hi, place) + dot(rest_lo, place)
    fold_ref[:, DEPTH - LANES :] = rest * tab_ref[3, pl.ds(HALF, 1), :]
    fold_hi, fold_lo = split(fold_ref[...])
    below = iota((32, DEPTH), 1) < DEPTH - MAIN
    both = jnp.concatenate([fold_hi, jnp.where(below, fold_lo, jnp.zeros_like(fold_lo))], axis=0)
    main_hi = fold_hi[:, : DEPTH - LANES]
    back_ref[...] = jnp.zeros(back_ref.shape, f32)
    tables = [None] * SLOTS
    spectra = [None] * SLOTS
    for s in KEPT + SENT:
        if s == SENT[0]:
            for copy in copies:
                copy.wait()
        rows = pl.ds(SLOT_BASE[s], DEGREES[s])
        ref = near_ref if s in KEPT else far_ref
        phi = jnp.concatenate([ref[b, rows, :] for b in (*range(HALF), 2 * HALF)], axis=1)
        plo = jnp.concatenate([ref[HALF + b, rows, :] for b in range(HALF)], axis=1)
        tables[s] = phi, plo
        main = dot_nt(both, phi)
        spectra[s] = main[:32] + (main[32:] + dot_nt(main_hi, plo))
    for s in range(SLOTS):
        count = DEGREES[s]
        phi, plo = tables[s]
        terms = spectra[s]
        degree = iota((1, count), 1)
        even = ((degree + device) & 1) == 0
        weight = 2.0 if s else jnp.where(device == 0, 1.0, 2.0)
        factor = resp_ref[:, DEVICES * s :] * weight
        real = jnp.where(even, terms[s : s + 1], terms[16 + s : 17 + s]) * factor
        imag = jnp.where(even, terms[8 + s : 9 + s], terms[24 + s : 25 + s]) * factor
        four = jnp.concatenate(
            [
                jnp.where(even, real, 0.0),
                jnp.where(even, imag, 0.0),
                jnp.where(even, 0.0, real),
                jnp.where(even, 0.0, imag),
                jnp.zeros((4, count), f32),
            ],
            axis=0,
        )
        hi, lo = split(four)
        out = dot(jnp.concatenate([hi, lo], axis=0), phi)
        both_rest = out[:8, DEPTH - LANES :]
        lower = jnp.concatenate([dot(hi, plo), pltpu.roll(both_rest, MAIN, 1)], axis=1)
        sums = out[:8] + (out[8:] + lower)
        for c in range(2):
            back_ref[pl.ds(8 * c + s, 1), :] = sums[c : c + 1] + sums[2 + c : 3 + c]
            back_ref[pl.ds(16 + 8 * c + s, 1), :] = sums[c : c + 1] - sums[2 + c : 3 + c]
    packed = back_ref[:, DEPTH - LANES :]
    group = iota((32, LANES), 1) // REST
    rest_hi, rest_lo = split(
        jnp.concatenate([jnp.where(group == g, packed, 0.0) for g in range(LAT)], axis=0)
    )
    rest = dot(rest_hi, spreader) + dot(rest_lo, spreader)
    for p in range(2):
        for y in range(HALF):
            band = y if p == 0 else LAT - 1 - y
            lanes = slice(LANES * y, LANES * (y + 1))
            real = back_ref[pl.ds(16 * p, ROWS), lanes]
            imag = back_ref[pl.ds(16 * p + 8, ROWS), lanes]
            for c in range(2):
                row = block * c + ROWS * band
                if c == 0:
                    sum_ref[pl.ds(row, ROWS), :] = jnp.where(first, real, pltpu.roll(imag, MAIN, 1))
                else:
                    sum_ref[pl.ds(row, ROWS), :] = jnp.where(first, pltpu.roll(real, MAIN, 1), imag)
                row_of = 32 * (2 * y + c) + 16 * p
                kept = jnp.where(own, rest[row_of : row_of + 16], 0.0)
                sum_ref[pl.ds(row + SLOTS, 1), :] = jnp.sum(kept, axis=0, keepdims=True)
    for c in range(2):
        total = sum_ref[pl.ds(block * c, block), :]
        for i in range(PAIRS):
            o_ref[pl.ds(block * (2 * i + c), block), :] = total


def half_inverse(ref, cos, sin, whi_ref, wlo_ref):
    lane = iota((DEVICES, LANES), 1)
    is_main = lane < MAIN
    is_rest = lane // REST == MAIN // REST
    rest = ref[pl.ds(SLOTS, DEVICES, stride=ROWS), :]
    total = None
    for s in range(SLOTS):
        main = ref[pl.ds(s, DEVICES, stride=ROWS), :]
        parts = []
        for c in range(2):
            shift = (MAIN - REST * (s + 8 * c)) % LANES
            moved = pltpu.roll(rest, shift, 1) if shift else rest
            body = pltpu.roll(main, MAIN, 1) if c else main
            parts.append(jnp.where(is_main, body, jnp.where(is_rest, moved, 0.0)))
        real, imag = parts
        pair = jnp.concatenate(split(jnp.concatenate([real * cos - imag * sin, real * sin + imag * cos], axis=0)), axis=1)
        whi = whi_ref[:, 256 * s : 256 * (s + 1)]
        wlo = wlo_ref[:, 256 * s : 256 * (s + 1)]
        terms = dot(whi, pair) + dot(wlo, pair)
        total = terms if total is None else total + terms
    return total[:, :LANES] + total[:, LANES:]


def in_rows(heights):
    north = lax.axis_index("lat") < HALF
    row = iota((PART, LANES), 0)
    order = ones_where(iota((PART, LANES), 1) == jnp.where(north, row, PART - 1 - row))
    first = heights.astype(bf16)
    second, third = split(heights - first.astype(f32))
    return dot_nt(order, first) + (dot_nt(order, second) + dot_nt(order, third))


def own_inverse_kernel(r_ref, base_ref, turn_ref, o_ref, phase_ref, whi_ref, wlo_ref):
    base_cos = base_ref[:, :DEVICES]
    base_sin = base_ref[:, DEVICES:]
    for s in range(SLOTS):
        wave = (base_cos, base_sin)
        if s:
            turn_cos = turn_ref[pl.ds(2 * s * TURN, TURN), :]
            turn_sin = turn_ref[pl.ds((2 * s + 1) * TURN, TURN), :]
            turn_cos = jnp.concatenate([turn_cos] * (CELLS // TURN), axis=0)
            turn_sin = jnp.concatenate([turn_sin] * (CELLS // TURN), axis=0)
            wave = (base_cos * turn_cos + base_sin * turn_sin, base_sin * turn_cos - base_cos * turn_sin)
        whi, wlo = split(jnp.concatenate(wave, axis=1))
        whi_ref[:, 256 * s : 256 * (s + 1)] = whi
        wlo_ref[:, 256 * s : 256 * (s + 1)] = wlo
    cos, sin = phases(lax.axis_index("lon"))
    phase_ref[0] = cos
    phase_ref[1] = sin
    o_ref[...] = in_rows(half_inverse(r_ref, cos, sin, whi_ref, wlo_ref))


def inverse_kernel(g_ref, own_ref, phase_ref, whi_ref, wlo_ref, o_hbm, got_ref, sems):
    part = lax.axis_index("lon") & 1
    north = lax.axis_index("lat") < HALF
    own_first = pl.multiple_of(PART * jnp.where(north, part, 1 - part), 8)
    got_first = pl.multiple_of(PART * jnp.where(north, 1 - part, part), 8)
    own_copy = pltpu.make_async_copy(own_ref, o_hbm.at[0, pl.ds(own_first, PART)], sems.at[0])
    got_copy = pltpu.make_async_copy(got_ref, o_hbm.at[0, pl.ds(got_first, PART)], sems.at[1])
    own_copy.start()
    got_ref[...] = in_rows(half_inverse(g_ref, phase_ref[0], phase_ref[1], whi_ref, wlo_ref))
    got_copy.start()
    own_copy.wait()
    got_copy.wait()


def vmem(n):
    return [pl.BlockSpec(memory_space=pltpu.VMEM)] * n


def hbm(n):
    return [pl.BlockSpec(memory_space=pltpu.HBM)] * n


def limit(mib):
    return pltpu.CompilerParams(vmem_limit_bytes=mib * 2**20)


def in_hbm(x):
    return pltpu.with_memory_space_constraint(jnp.asarray(x), pltpu.HBM)


def swapped(x):
    return lax.ppermute(x, "lon", [(i, i ^ 1) for i in range(LON)])


def exchanged(x):
    x = x.reshape(DEVICES, 1, ROWS * LANES)
    x = lax.all_to_all(x, ("lon", "lat"), split_axis=0, concat_axis=0, tiled=True)
    return x.reshape(DEVICES * ROWS, LANES)


def recurrence_factors(device):
    degree = jnp.arange(MODES, dtype=jnp.int32)[None, :]
    order = (device + DEVICES * jnp.arange(SLOTS, dtype=jnp.int32))[:, None]
    started = degree > order
    l = degree.astype(f32)
    m = order.astype(f32)
    k = l - 1.0
    growth = jnp.where(started, jnp.sqrt((4.0 * l * l - 1.0) / jnp.where(started, l * l - m * m, 1.0)), 0.0)
    damping = jnp.sqrt(jnp.where(started, k * k - m * m, 0.0) / jnp.maximum(4.0 * k * k - 1.0, 1.0))
    return jnp.stack([growth, growth * damping]).reshape(2 * SLOTS * MODES)


def shards(height, response):
    device = lax.axis_index("lon") * LAT + lax.axis_index("lat")
    table = wave_table()
    tables = jnp.asarray(row_tables())
    packed = jax.ShapeDtypeStruct((DEVICES * ROWS, LANES), f32)
    got = swapped(height)
    kept = jax.ShapeDtypeStruct((2 * HALF + 1, KEPT_ROWS, LANES), bf16)
    sent = pltpu.HBM((2 * HALF + 1, SENT_ROWS, LANES), bf16)
    far = [pltpu.VMEM((2 * HALF + 1, SENT_ROWS, LANES), bf16)]
    near_legendre, far_legendre = pl.pallas_call(
        legendre_kernel,
        out_shape=(kept, sent),
        in_specs=[pl.BlockSpec(memory_space=pltpu.SMEM)] + vmem(1),
        out_specs=tuple(vmem(1) + hbm(1)),
        scratch_shapes=far
        + [
            pltpu.VMEM((SLOTS * DEVICES * 8, LANES), f32),
            pltpu.SemaphoreType.DMA((SLOTS, len(SENT))),
        ],
        compiler_params=limit(16),
        name="legendre",
    )(recurrence_factors(device), tables)
    operand = jax.ShapeDtypeStruct((LANES, CELLS), bf16)
    waves = jax.ShapeDtypeStruct((2 * MODES, CELLS), bf16)
    own_half = pl.pallas_call(
        own_kernel,
        out_shape=(
            operand,
            operand,
            waves,
            waves,
            jax.ShapeDtypeStruct((4, 16, LANES), f32),
            jax.ShapeDtypeStruct((LANES, BAND), bf16),
        ),
        in_specs=hbm(2),
        out_specs=tuple(vmem(6)),
        scratch_shapes=[
            pltpu.VMEM((1, BAND, CELLS), f32),
            pltpu.VMEM((2 * DEVICES + 16, CELLS), f32),
            pltpu.SemaphoreType.DMA((2,)),
        ],
        compiler_params=limit(12),
        name="own_half",
    )(in_hbm(height), in_hbm(first_waves(table)))
    shares = pl.pallas_call(
        forward_kernel,
        out_shape=packed,
        in_specs=vmem(7),
        out_specs=vmem(1)[0],
        compiler_params=limit(12),
        name="forward_dft",
    )(got, *own_half)
    arrived = exchanged(shares)
    synthesis = pl.pallas_call(
        degree_kernel,
        out_shape=packed,
        in_specs=vmem(2) + hbm(1) + vmem(2),
        out_specs=vmem(1)[0],
        scratch_shapes=far
        + [
            pltpu.VMEM((2 * LAT * ROWS, LANES), f32),
            pltpu.VMEM((32, DEPTH), f32),
            pltpu.VMEM((32, LAT * LANES), f32),
            pltpu.VMEM((32, DEPTH), f32),
            pltpu.SemaphoreType.DMA((len(SENT),)),
        ],
        compiler_params=limit(16),
        name="degrees",
    )(arrived, near_legendre, in_hbm(far_legendre), tables, response.reshape(1, MODES))
    returned = exchanged(synthesis)
    other = swapped(returned)
    waves = jax.ShapeDtypeStruct((CELLS, 2 * MODES), bf16)
    base, turns = last_waves(table)
    own, phase, thi, tlo = pl.pallas_call(
        own_inverse_kernel,
        out_shape=(
            jax.ShapeDtypeStruct((PART, CELLS), f32),
            jax.ShapeDtypeStruct((2, DEVICES, LANES), f32),
            waves,
            waves,
        ),
        in_specs=vmem(3),
        out_specs=tuple(vmem(4)),
        compiler_params=limit(12),
        name="own_inverse_dft",
    )(returned, jnp.asarray(base), jnp.asarray(turns))
    return pl.pallas_call(
        inverse_kernel,
        out_shape=jax.ShapeDtypeStruct((1, BAND, CELLS), f32),
        in_specs=vmem(5),
        out_specs=hbm(1)[0],
        scratch_shapes=[pltpu.VMEM((PART, CELLS), f32), pltpu.SemaphoreType.DMA((2,))],
        compiler_params=limit(12),
        name="inverse_dft",
    )(other, own, phase, thi, tlo)


def solution(mesh):
    placed = (P(None, "lat", "lon"), P())
    return jax.shard_map(
        shards, mesh=mesh, in_specs=placed, out_specs=P(None, "lat", "lon"), check_vma=False
    )
```
